32 devices in a mesh: groups: 2 (over x), row: 16 (over z, y, core), col: 1.
Axes of the slice: x: 2, y: 2, z: 4, core: 2. Of those that a mesh axis runs over, the one named last changes fastest.
Arguments:
- pair_rep: bfloat16 [256, 128, 128], P(('groups', 'row'), 'col'), parts along dimension 0, may hold values from -6 to 6
- residue_mask: int32 [256], P('groups'), parts along dimension 0, may hold values 0 or 1
- crop_length: int32 [2], P('groups'), parts along dimension 0, may hold values from 64 to 128
- norm_gain: float32 [2, 128], replicated, may hold values from 0.25 to 1.75
- mult_proj: bfloat16 [2, 128, 640], replicated, may hold values from -0.5 to 0.5
- mixed_gain: float32 [2, 128], replicated, may hold values from 0.25 to 1.75
- mult_out: bfloat16 [2, 128, 128], replicated, may hold values from -0.5 to 0.5
- att_gain: float32 [128], replicated, may hold values from 0.25 to 1.75
- att_proj: bfloat16 [128, 512], replicated, may hold values from -5 to 5
- att_bias: bfloat16 [128, 4], replicated, may hold values from -0.5 to 0.5
- att_out: bfloat16 [128, 128], replicated, may hold values from -0.5 to 0.5
Outputs:
- pair_out: bfloat16 [256, 128, 128], P(('groups', 'row'), 'col'), parts along dimension 0
The draws below stay inside these ranges and needn't reach their ends.
There are 2 independent parts, one for each index of `groups`. The reference program is written for one: setup_inputs(seed, part) draws one part's arguments, and reference() takes and returns one part's arrays. A program takes and returns all parts, laid end to end along the dimension named above; an argument that names none is the same for every part. Nothing has to cross between parts.
All inputs are finite; a program needn't handle non-finite values.
Results may differ from the reference program's by a relative error of at most 0.03.
Values may be sent and summed in bfloat16 or wider, within the bound.
A program may use at most 64 MiB of HBM per device.

```python
import jax
import jax.numpy as jnp
from jax import lax

C = 128
HID = 128
HEADS = 4
HEAD_DIM = 32
ATT = 128
NRES = 128


def draw_att_proj(key, part):
    drawn = jax.random.normal(key, (C, 4 * ATT), jnp.float32) * C ** (-0.5)
    return jnp.clip(drawn, -5.0, 5.0).astype(jnp.bfloat16)


def touch_ends(values, stream_key, smallest, top_value):
    longest = values.shape.index(max(values.shape))
    spots = []
    for shift in (0, 1):
        where = [jax.random.randint(jax.random.fold_in(stream_key, axis), (), 0, length) for axis, length in enumerate(values.shape)]
        where[longest] = (where[longest] + shift) % values.shape[longest]
        spots.append(tuple(where))
    return values.at[spots[0]].set(smallest).at[spots[1]].set(top_value)


def block_scale(own_key, dims, pieces, smallest, top_value):
    def one(position, shards_of):
        heights = jax.random.uniform(jax.random.fold_in(jax.random.fold_in(own_key, 6), position), (shards_of,), jnp.float32, smallest / len(pieces), top_value / len(pieces))
        return jnp.repeat(jnp.exp(heights), dims[position] // shards_of).reshape((-1,) + (1,) * (len(dims) - position - 1))

    level = one(*pieces[0])
    for cut in pieces[1:]:
        level = level * one(*cut)
    return level


def centred(own_key, dims, deviation, reach, split=(), kind=jnp.bfloat16):
    entries = deviation * jax.random.normal(own_key, dims, jnp.float32)
    if split:
        entries = entries * block_scale(own_key, dims, split, -0.22, 0.18)
    return jnp.clip(entries, -reach, reach).astype(kind)


def setup_inputs(seed: int = 0, part: int = 0) -> dict:
    arg_keys = jax.random.split(jax.random.key(seed), 12)
    part_splits = jax.random.split(jax.random.fold_in(arg_keys[11], part), 12)
    pair_rep = centred(part_splits[0], (NRES, NRES, C), 1.0, 6.0, ((0, 16),))
    residue_mask = touch_ends((jax.random.randint(part_splits[1], (NRES,), 0, 8) < 7).astype(jnp.int32), jax.random.fold_in(part_splits[1], 1), 0, 1)
    crop_length = jax.random.randint(part_splits[2], (1,), NRES // 2, NRES + 1).astype(jnp.int32)
    norm_gain = jnp.clip(1.0 + 0.15 * jax.random.normal(arg_keys[3], (2, C), jnp.float32), 0.25, 1.75)
    mult_proj = centred(arg_keys[4], (2, C, 4 * HID + C), C ** -0.5, 0.5)
    mixed_gain = jnp.clip(1.0 + 0.15 * jax.random.normal(arg_keys[5], (2, HID), jnp.float32), 0.25, 1.75)
    mult_out = centred(arg_keys[6], (2, HID, C), HID ** -0.5, 0.5)
    att_gain = jnp.clip(1.0 + 0.15 * jax.random.normal(arg_keys[7], (C,), jnp.float32), 0.25, 1.75)
    att_proj = draw_att_proj(jax.random.fold_in(arg_keys[11], 71), part)
    att_bias = centred(arg_keys[9], (C, HEADS), C ** -0.5, 0.5)
    att_out = centred(arg_keys[10], (ATT, C), ATT ** -0.5, 0.5)
    return dict(pair_rep=pair_rep, residue_mask=residue_mask, crop_length=crop_length, norm_gain=norm_gain, mult_proj=mult_proj, mixed_gain=mixed_gain, mult_out=mult_out, att_gain=att_gain, att_proj=att_proj, att_bias=att_bias, att_out=att_out)


EPSILON = 1e-05

def normalize(values, gain_vec, along):
    average = lax.optimization_barrier(jnp.mean(values, axis=along, keepdims=True))
    centered = values - average
    variance = lax.optimization_barrier(jnp.mean(centered * centered, axis=along, keepdims=True))
    return centered * lax.rsqrt(variance + EPSILON) * gain_vec

def live_mask(residue_mask, crop_length):
    positions = jnp.arange(residue_mask.shape[0], dtype=jnp.int32)
    alive = ((residue_mask == 1) | (positions == 0)) & (positions < crop_length[0])
    return alive.astype(jnp.float32)

def triangle_update(pair_rep, gain_vec, proj_w, out_gain, out_w, pair_mask, incoming):
    normed = normalize(pair_rep.astype(jnp.float32), gain_vec, -1).astype(jnp.bfloat16)
    projected = jnp.dot(normed.reshape(-1, C), proj_w, preferred_element_type=jnp.float32)
    projected = projected.reshape(NRES, NRES, 4 * HID + C)
    masked = pair_mask[:, :, None]
    left_proj = (masked * jax.nn.sigmoid(projected[..., HID:2 * HID]) * projected[..., :HID]).astype(jnp.bfloat16)
    right_proj = (masked * jax.nn.sigmoid(projected[..., 3 * HID:4 * HID]) * projected[..., 2 * HID:3 * HID]).astype(jnp.bfloat16)
    gate_lin = projected[..., 4 * HID:]
    if incoming:
        product = jnp.einsum('kic,kjc->ijc', left_proj.astype(jnp.float32), right_proj.astype(jnp.float32))
    else:
        product = jnp.einsum('ikc,jkc->ijc', left_proj.astype(jnp.float32), right_proj.astype(jnp.float32))
    mixed = product.astype(jnp.bfloat16)
    mixed_norm = normalize(mixed.astype(jnp.float32), out_gain, -1).astype(jnp.bfloat16)
    update = jnp.dot(mixed_norm.reshape(-1, HID), out_w, preferred_element_type=jnp.float32).reshape(NRES, NRES, C)
    return (pair_rep.astype(jnp.float32) + jax.nn.sigmoid(gate_lin) * update).astype(jnp.bfloat16)

def reference(pair_rep, residue_mask, crop_length, norm_gain, mult_proj, mixed_gain, mult_out, att_gain, att_proj, att_bias, att_out):
    alive = live_mask(residue_mask, crop_length)
    pair_mask = alive[:, None] * alive[None, :]
    first = triangle_update(pair_rep, norm_gain[0], mult_proj[0], mixed_gain[0], mult_out[0], pair_mask, False)
    second = triangle_update(first, norm_gain[1], mult_proj[1], mixed_gain[1], mult_out[1], pair_mask, True)
    normed = normalize(second.astype(jnp.float32), att_gain, -1).astype(jnp.bfloat16)
    projected = jnp.dot(normed.reshape(-1, C), att_proj, preferred_element_type=jnp.float32).reshape(NRES, NRES, 4 * ATT)
    queries = projected[..., :ATT].astype(jnp.bfloat16)
    key_rows = projected[..., ATT:2 * ATT].astype(jnp.bfloat16)
    value_rows = projected[..., 2 * ATT:3 * ATT].astype(jnp.bfloat16)
    gates = projected[..., 3 * ATT:].astype(jnp.bfloat16)
    tri_bias = jnp.dot(normed.reshape(-1, C), att_bias, preferred_element_type=jnp.float32)
    tri_bias = tri_bias.astype(jnp.bfloat16).reshape(NRES, NRES, HEADS)
    bias_heads = jnp.transpose(tri_bias.astype(jnp.float32), (2, 0, 1))
    key_mask = jnp.where(alive > 0, 0.0, -1000000000.0).astype(jnp.float32)
    scaling = 1.0 / math_sqrt(HEAD_DIM)

    def one_row(items):
        query_row, key_row, value_row, gate_row = items
        query_row = query_row.reshape(NRES, HEADS, HEAD_DIM).astype(jnp.float32)
        key_row = key_row.reshape(NRES, HEADS, HEAD_DIM).astype(jnp.float32)
        value_row = value_row.reshape(NRES, HEADS, HEAD_DIM).astype(jnp.float32)
        scores = jnp.einsum('jhd,khd->hjk', query_row, key_row) * scaling + bias_heads + key_mask[None, None, :]
        weights = jax.nn.softmax(scores, axis=-1).astype(jnp.bfloat16)
        attended = jnp.einsum('hjk,khd->jhd', weights.astype(jnp.float32), value_row).reshape(NRES, ATT)
        return (jax.nn.sigmoid(gate_row.astype(jnp.float32)) * attended).astype(jnp.bfloat16)
    gated = lax.map(one_row, (queries, key_rows, value_rows, gates))
    result = jnp.dot(gated.reshape(-1, ATT), att_out, preferred_element_type=jnp.float32).reshape(NRES, NRES, C)
    return (second.astype(jnp.float32) + result).astype(jnp.bfloat16)

def math_sqrt(number):
    return float(number) ** 0.5
```

```python
import functools

import jax
import jax.numpy as jnp
from jax import lax
from jax.experimental import pallas as pl
from jax.experimental.pallas import tpu as pltpu
from jax.sharding import PartitionSpec as P

HID = 128
HEADS = 4
HEAD_DIM = 32
ATT = 128


EPSILON = 1e-05


def normalize(values, gain_vec, along):
    average = jnp.mean(values, axis=along, keepdims=True)
    centered = values - average
    variance = jnp.mean(centered * centered, axis=along, keepdims=True)
    return centered * lax.rsqrt(variance + EPSILON) * gain_vec


def outgoing_product(left_half, right_half):
    return lax.dot_general(
        left_half,
        lax.all_gather(right_half, "row", axis=1, tiled=True),
        (((2,), (2,)), ((0,), (0,))),
        preferred_element_type=jnp.float32,
    )


def incoming_product(left_half, right_half):
    left_cols, right_cols = (
        lax.all_to_all(left_half, "row", split_axis=2, concat_axis=1, tiled=True),
        lax.all_to_all(right_half, "row", split_axis=2, concat_axis=1, tiled=True),
    )
    return lax.dot_general(
        left_cols,
        lax.all_gather(right_cols, "row", axis=2, tiled=True),
        (((1,), (1,)), ((0,), (0,))),
        preferred_element_type=jnp.float32,
    )


def triangle_update(pair_rep, gain_vec, proj_w, out_gain, out_w, pair_mask, incoming):
    normed = normalize(pair_rep.astype(jnp.float32), gain_vec, 2).astype(jnp.bfloat16)
    channels = jnp.einsum(
        "ijd,de->eij", normed, proj_w[:, : 4 * HID], preferred_element_type=jnp.float32
    )
    gate_lin = jnp.einsum(
        "ijd,de->ije", normed, proj_w[:, 4 * HID :], preferred_element_type=jnp.float32
    )
    masked = pair_mask[None, :, :]
    left_proj = (masked * jax.nn.sigmoid(channels[HID : 2 * HID]) * channels[:HID]).astype(
        jnp.bfloat16
    )
    right_proj = (
        masked * jax.nn.sigmoid(channels[3 * HID : 4 * HID]) * channels[2 * HID : 3 * HID]
    ).astype(jnp.bfloat16)
    left_half, right_half = (
        lax.all_to_all(left_proj, "col", split_axis=0, concat_axis=2, tiled=True),
        lax.all_to_all(right_proj, "col", split_axis=0, concat_axis=2, tiled=True),
    )
    if incoming:
        product = incoming_product(left_half, right_half)
    else:
        product = outgoing_product(left_half, right_half)
    mixed = product.astype(jnp.bfloat16)
    mixed_tile = lax.all_to_all(mixed, "col", split_axis=2, concat_axis=0, tiled=True)
    mixed_norm = normalize(mixed_tile.astype(jnp.float32), out_gain[:, None, None], 0).astype(
        jnp.bfloat16
    )
    update = jnp.einsum("cij,cd->ijd", mixed_norm, out_w, preferred_element_type=jnp.float32)
    return (pair_rep.astype(jnp.float32) + jax.nn.sigmoid(gate_lin) * update).astype(jnp.bfloat16)


def local(
    pair_rep,
    residue_mask,
    crop_length,
    norm_gain,
    mult_proj,
    mixed_gain,
    mult_out,
    att_gain,
    att_proj,
    att_bias,
    att_out,
):
    row_count = pair_rep.shape[0]
    col_count = pair_rep.shape[1]
    row_start = lax.axis_index("row") * row_count
    col_start = lax.axis_index("col") * col_count
    positions = jnp.arange(residue_mask.shape[0], dtype=jnp.int32)
    alive = (((residue_mask == 1) | (positions == 0)) & (positions < crop_length[0])).astype(
        jnp.float32
    )
    row_alive = lax.dynamic_slice_in_dim(alive, row_start, row_count, 0)
    col_alive = lax.dynamic_slice_in_dim(alive, col_start, col_count, 0)
    pair_mask = row_alive[:, None] * col_alive[None, :]
    first = triangle_update(
        pair_rep, norm_gain[0], mult_proj[0], mixed_gain[0], mult_out[0], pair_mask, False
    )
    second = triangle_update(
        first, norm_gain[1], mult_proj[1], mixed_gain[1], mult_out[1], pair_mask, True
    )
    normed = normalize(second.astype(jnp.float32), att_gain, 2).astype(jnp.bfloat16)
    projected = jnp.einsum("ijd,de->ije", normed, att_proj, preferred_element_type=jnp.float32)
    queries = projected[..., :ATT].astype(jnp.bfloat16)
    key_rows = projected[..., ATT : 2 * ATT].astype(jnp.bfloat16)
    value_rows = projected[..., 2 * ATT : 3 * ATT].astype(jnp.bfloat16)
    gates = projected[..., 3 * ATT :].astype(jnp.bfloat16)
    bias_tile = jnp.einsum(
        "ijd,dh->hij", normed, att_bias, preferred_element_type=jnp.float32
    ).astype(jnp.bfloat16)
    key_all, value_all, bias_cols = (
        lax.all_gather(key_rows, "col", axis=1, tiled=True),
        lax.all_gather(value_rows, "col", axis=1, tiled=True),
        lax.all_gather(bias_tile, "col", axis=2, tiled=True),
    )
    bias_full = lax.all_gather(bias_cols, "row", axis=1, tiled=True)
    bias_mine = lax.dynamic_slice_in_dim(bias_full, col_start, col_count, 1).astype(jnp.float32)
    total = key_all.shape[1]
    key_mask = jnp.where(alive > 0, 0.0, -1000000000.0).astype(jnp.float32)
    scaling = 1.0 / float(HEAD_DIM) ** 0.5
    query_heads = queries.reshape(row_count, col_count, HEADS, HEAD_DIM)
    key_heads = key_all.reshape(row_count, total, HEADS, HEAD_DIM)
    value_heads = value_all.reshape(row_count, total, HEADS, HEAD_DIM)
    scores = jnp.einsum(
        "ijhd,ikhd->hijk", query_heads, key_heads, preferred_element_type=jnp.float32
    )
    scores = scores * scaling + bias_mine[:, None, :, :] + key_mask[None, None, None, :]
    weights = jax.nn.softmax(scores, axis=-1).astype(jnp.bfloat16)
    attended = jnp.einsum(
        "hijk,ikhd->ijhd", weights, value_heads, preferred_element_type=jnp.float32
    )
    attended = attended.reshape(row_count, col_count, ATT)
    gated = (jax.nn.sigmoid(gates.astype(jnp.float32)) * attended).astype(jnp.bfloat16)
    result = jnp.einsum("ija,ad->ijd", gated, att_out, preferred_element_type=jnp.float32)
    return (second.astype(jnp.float32) + result).astype(jnp.bfloat16)


MESH = pl.DeviceIdType.MESH
BF16 = jnp.bfloat16
F32 = jnp.float32
GROUP = 8
PARTS = 1


def sigmoid(x):
    return 0.5 * jnp.tanh(0.5 * x) + 0.5


def normalize_t(values, gain_col):
    average = jnp.mean(values, axis=0, keepdims=True)
    centered = values - average
    variance = jnp.mean(centered * centered, axis=0, keepdims=True)
    return centered * lax.rsqrt(variance + EPSILON) * gain_col


def mm(a, b, dims=((1,), (0,))):
    return lax.dot_general(a, b, (dims, ((), ())), preferred_element_type=F32)


def fused_kernel(
    n,
    pair_ref,
    mask_ref,
    crop_ref,
    gain_ref,
    proj_ref,
    mgain_ref,
    mout_ref,
    again_ref,
    aproj_ref,
    abias_ref,
    aout_ref,
    out_ref,
    zt,
    og,
    f_left,
    f_right,
    fx_left,
    fx_right,
    f_prod,
    f_bias,
    b_pad,
    b_full,
    kmat,
    qvg,
    proj_t,
    out_t,
    gain_cols,
    qvg_t,
    send_lr,
    recv_lr,
    send_p,
    recv_p,
    send_b,
    recv_b,
    send_sem,
    recv_sem,
):
    me = lax.axis_index("row")
    rows, cols, chans = pair_ref.shape
    mine = chans // n
    block = rows * mine
    half = rows // PARTS
    hblock = half * mine
    heads = abias_ref.shape[0]
    att = chans
    hid = chans

    barrier = pltpu.get_barrier_semaphore()
    for s in range(1, n):
        pl.semaphore_signal(
            barrier, inc=1, device_id={"row": lax.rem(me + s, n)}, device_id_type=MESH
        )

    def column(row_vec):
        return jnp.transpose(jnp.broadcast_to(row_vec.astype(F32), (chans, row_vec.shape[-1])))

    def flip(mat):
        return jnp.transpose(mat.astype(F32)).astype(BF16)

    lane = lax.broadcasted_iota(jnp.int32, (1, cols), 1)
    alive = jnp.where(
        ((mask_ref[...] == 1) | (lane == 0)) & (lane < crop_ref[0]), 1.0, 0.0
    ).astype(F32)

    def row_mask(i):
        here = jnp.where(lane == me * rows + i, alive, 0.0)
        return jnp.sum(here, axis=1, keepdims=True) * alive

    masks = [row_mask(i) for i in range(rows)]

    def exchange(phase, src, dst, p, slot):
        return pltpu.make_async_remote_copy(
            src_ref=src.at[p],
            dst_ref=dst.at[slot],
            send_sem=send_sem.at[phase, p],
            recv_sem=recv_sem.at[phase, slot],
            device_id={"row": p},
            device_id_type=MESH,
        )

    def send_all(phase, src, dst):
        for s in range(1, n):
            exchange(phase, src, dst, lax.rem(me + s, n), me).start()

    def take_all(phase, src, dst):
        for s in range(1, n):
            q = lax.rem(me + n - s, n)
            exchange(phase, src, dst, q, q).wait_recv()

    def at_row(i):
        return slice(i * cols, (i + 1) * cols)

    def lr_phase(u, k):
        return u * 2 * PARTS + k

    def p_phase(u, k):
        return u * 2 * PARTS + PARTS + k

    def b_phase(k):
        return 4 * PARTS + k

    def project(u, k):
        for i in range(k * half, (k + 1) * half):
            normed = normalize_t(zt[:, at_row(i)].astype(F32), gain_cols[u]).astype(BF16)
            pr = mm(proj_t[u], normed)
            left = masks[i] * sigmoid(pr[hid : 2 * hid]) * pr[:hid]
            right = masks[i] * sigmoid(pr[3 * hid : 4 * hid]) * pr[2 * hid : 3 * hid]
            f_left[:, i] = left.reshape(n, mine, cols)
            f_right[:, i] = right.reshape(n, mine, cols)
            og[:, at_row(i)] = sigmoid(pr[4 * hid :])
        src, dst = send_lr.at[u, k], recv_lr.at[u, k]
        for p in range(n):
            at = slice(k * half, (k + 1) * half)
            src[p, 0] = f_left[p, at].reshape(hblock, cols).astype(BF16)
            src[p, 1] = f_right[p, at].reshape(hblock, cols).astype(BF16)
        if u == 0 and k == 0:
            pl.semaphore_wait(barrier, n - 1)
        send_all(lr_phase(u, k), src, dst)
        dst[me] = src[me]

    def multiply(u):
        for k in range(PARTS):
            src, dst = send_lr.at[u, k], recv_lr.at[u, k]
            take_all(lr_phase(u, k), src, dst)
            for q in range(n):
                at = pl.ds(q * block + k * hblock, hblock)
                fx_left[at, :] = dst[q, 0].astype(F32)
                fx_right[at, :] = dst[q, 1].astype(F32)
        for c in range(mine):
            at = pl.ds(c, n * rows, stride=mine)
            a = fx_left[at, :].astype(BF16)
            b = fx_right[at, :].astype(BF16)
            if u == 0:
                f_prod[at, :] = mm(a, b, ((1,), (1,)))
            else:
                f_prod[at, :] = mm(a, b, ((0,), (0,)))
        for k in range(PARTS):
            src, dst = send_p.at[u, k], recv_p.at[u, k]
            for p in range(n):
                src[p] = f_prod[pl.ds(p * block + k * hblock, hblock), :].astype(BF16)
            send_all(p_phase(u, k), src, dst)
            dst[me] = src[me]

    def finish(u, k):
        src, dst = send_p.at[u, k], recv_p.at[u, k]
        take_all(p_phase(u, k), src, dst)
        for q in range(n):
            f_left[q, k * half : (k + 1) * half] = dst[q].astype(F32).reshape(half, mine, cols)
        for i in range(k * half, (k + 1) * half):
            at = at_row(i)
            mixed = f_left[:, i].reshape(chans, cols)
            mixed_norm = normalize_t(mixed, gain_cols[2 + u]).astype(BF16)
            zt[:, at] = (zt[:, at].astype(F32) + og[:, at] * mm(out_t[u], mixed_norm)).astype(BF16)

    def bias_copy(k, p, slot):
        return pltpu.make_async_remote_copy(
            src_ref=send_b.at[k],
            dst_ref=recv_b.at[k, slot],
            send_sem=send_sem.at[b_phase(k), p],
            recv_sem=recv_sem.at[b_phase(k), slot],
            device_id={"row": p},
            device_id_type=MESH,
        )

    def attention_inputs(k):
        normed_rows = []
        for i in range(k * half, (k + 1) * half):
            normed = normalize_t(zt[:, at_row(i)].astype(F32), gain_cols[4]).astype(BF16)
            normed_rows.append(normed)
            bias_row = mm(b_pad[...].astype(BF16), normed)
            for h in range(heads):
                f_bias[k, h * half + i - k * half : h * half + i - k * half + 1, :] = bias_row[h : h + 1, :]
        send_b[k] = f_bias[k].astype(BF16)
        for s in range(1, n):
            bias_copy(k, lax.rem(me + s, n), me).start()
        recv_b[k, me] = f_bias[k].astype(BF16)
        for i in range(k * half, (k + 1) * half):
            normed = normed_rows[i - k * half]
            kmat[i] = mm(flip(normed), aproj_ref[:, att : 2 * att]).astype(BF16)
            qvg[i] = mm(qvg_t[...], normed).astype(BF16)

    gain_cols[0] = column(gain_ref[0:1, :])
    proj_t[0] = flip(proj_ref[0])
    for i in range(rows):
        zt[:, at_row(i)] = flip(pair_ref[i])
    for k in range(PARTS):
        project(0, k)
    gain_cols[1] = column(gain_ref[1:2, :])
    gain_cols[2] = column(mgain_ref[0:1, :])
    gain_cols[3] = column(mgain_ref[1:2, :])
    gain_cols[4] = column(again_ref[...])
    proj_t[1] = flip(proj_ref[1])
    for u in range(2):
        out_t[u] = flip(mout_ref[u])
    out_t[2] = flip(aout_ref[...])
    qvg_t[:att] = flip(aproj_ref[:, :att])
    qvg_t[att:] = flip(aproj_ref[:, 2 * att :])
    b_pad[...] = jnp.zeros_like(b_pad)
    b_pad[:heads] = abias_ref[...].astype(F32)
    key_mask = column(jnp.where(alive > 0, 0.0, -1000000000.0))
    multiply(0)
    for k in range(PARTS):
        finish(0, k)
        project(1, k)
    multiply(1)
    for k in range(PARTS):
        finish(1, k)
        attention_inputs(k)

    for k in range(PARTS):
        for s in range(1, n):
            q = lax.rem(me + n - s, n)
            bias_copy(k, q, q).wait_recv()
    for h in range(heads):
        pieces = []
        for q in range(n):
            for k in range(PARTS):
                pieces.append(recv_b[k, q].astype(F32)[h * half : (h + 1) * half])
        b_full[h] = jnp.transpose(jnp.concatenate(pieces, axis=0)) + key_mask
    dim = att // heads
    scaling = 1.0 / float(dim) ** 0.5

    def attend(i, carry):
        parts = []
        for h in range(heads):
            ch = slice(h * dim, (h + 1) * dim)
            scores = mm(kmat[i, :, ch], qvg[i, ch, :]) * scaling + b_full[h]
            top = jnp.max(scores, axis=0, keepdims=True)
            e = jnp.exp(scores - top)
            w = (e * (1.0 / jnp.sum(e, axis=0, keepdims=True))).astype(BF16)
            parts.append(mm(qvg[i, att + h * dim : att + (h + 1) * dim, :], w))
        attended = jnp.concatenate(parts, axis=0)
        gated = (sigmoid(qvg[i, 2 * att :, :].astype(F32)) * attended).astype(BF16)
        result = mm(out_t[2], gated)
        at = pl.ds(pl.multiple_of(i * cols, cols), cols)
        out_ref[i] = jnp.transpose(zt[:, at].astype(F32) + result).astype(BF16)
        return carry

    lax.fori_loop(0, rows, attend, 0, unroll=4)

    def drain(s, carry):
        p = lax.rem(me + s, n)
        for k in range(PARTS):
            for u in range(2):
                exchange(lr_phase(u, k), send_lr.at[u, k], recv_lr.at[u, k], p, me).wait_send()
                exchange(p_phase(u, k), send_p.at[u, k], recv_p.at[u, k], p, me).wait_send()
            bias_copy(k, p, me).wait_send()
        return carry

    lax.fori_loop(1, n, drain, 0)


def fused(n, pair_rep, residue_mask, crop_length, norm_gain, mult_proj, mixed_gain, mult_out,
          att_gain, att_proj, att_bias, att_out):
    rows, cols, chans = pair_rep.shape
    heads = att_bias.shape[1]
    mine = chans // n
    block = rows * mine
    hblock = block // PARTS
    vm = pl.BlockSpec(memory_space=pltpu.VMEM)
    sm = pl.BlockSpec(memory_space=pltpu.SMEM)
    big = n * block
    return pl.pallas_call(
        functools.partial(fused_kernel, n),
        out_shape=jax.ShapeDtypeStruct(pair_rep.shape, BF16),
        in_specs=[vm, vm, sm] + [vm] * 8,
        out_specs=vm,
        scratch_shapes=[
            pltpu.VMEM((chans, rows * cols), BF16),
            pltpu.VMEM((chans, rows * cols), F32),
            pltpu.VMEM((n, rows, mine, cols), F32),
            pltpu.VMEM((n, rows, mine, cols), F32),
            pltpu.VMEM((big, cols), F32),
            pltpu.VMEM((big, cols), F32),
            pltpu.VMEM((big, cols), F32),
            pltpu.VMEM((PARTS, heads * rows // PARTS, cols), F32),
            pltpu.VMEM((2 * GROUP, chans), F32),
            pltpu.VMEM((heads, cols, cols), F32),
            pltpu.VMEM((rows, cols, chans), BF16),
            pltpu.VMEM((rows, 3 * chans, cols), BF16),
            pltpu.VMEM((2, mult_proj.shape[2], chans), BF16),
            pltpu.VMEM((3, chans, chans), BF16),
            pltpu.VMEM((5, chans, cols), F32),
            pltpu.VMEM((3 * chans, chans), BF16),
            pltpu.VMEM((2, PARTS, n, 2, hblock, cols), BF16),
            pltpu.VMEM((2, PARTS, n, 2, hblock, cols), BF16),
            pltpu.VMEM((2, PARTS, n, hblock, cols), BF16),
            pltpu.VMEM((2, PARTS, n, hblock, cols), BF16),
            pltpu.VMEM((PARTS, heads * rows // PARTS, cols), BF16),
            pltpu.VMEM((PARTS, n, heads * rows // PARTS, cols), BF16),
            pltpu.SemaphoreType.DMA((5 * PARTS, n)),
            pltpu.SemaphoreType.DMA((5 * PARTS, n)),
        ],
        compiler_params=pltpu.CompilerParams(
            collective_id=0, has_side_effects=True, vmem_limit_bytes=48 * 1024 * 1024
        ),
        name="fused_pair",
    )(
        pair_rep,
        residue_mask.reshape(1, -1),
        crop_length,
        norm_gain,
        mult_proj,
        mixed_gain,
        mult_out,
        att_gain.reshape(1, -1),
        att_proj,
        att_bias.T,
        att_out,
    )


def choose(mesh):
    n = mesh.shape["row"]

    def body(pair_rep, *rest):
        rows, cols, chans = pair_rep.shape
        fits = (
            mesh.shape["col"] == 1
            and chans == n * GROUP
            and rows == GROUP
            and cols == n * rows
            and cols == chans
        )
        if fits:
            return fused(n, pair_rep, *rest)
        return local(pair_rep, *rest)

    return body


def solution(mesh):
    placed = (
        P(("groups", "row"), "col", None),
        P("groups"),
        P("groups"),
        P(),
        P(),
        P(),
        P(),
        P(),
        P(),
        P(),
        P(),
    )
    return jax.shard_map(
        choose(mesh),
        mesh=mesh,
        in_specs=placed,
        out_specs=P(("groups", "row"), "col", None),
        check_vma=False,
    )
```

```python
import functools

import jax
import jax.numpy as jnp
from jax import lax
from jax.experimental import pallas as pl
from jax.experimental.pallas import tpu as pltpu
from jax.sharding import PartitionSpec as P

HID = 128
HEADS = 4
HEAD_DIM = 32
ATT = 128


EPSILON = 1e-05


def normalize(values, gain_vec, along):
    average = jnp.mean(values, axis=along, keepdims=True)
    centered = values - average
    variance = jnp.mean(centered * centered, axis=along, keepdims=True)
    return centered * lax.rsqrt(variance + EPSILON) * gain_vec


def outgoing_product(left_half, right_half):
    return lax.dot_general(
        left_half,
        lax.all_gather(right_half, "row", axis=1, tiled=True),
        (((2,), (2,)), ((0,), (0,))),
        preferred_element_type=jnp.float32,
    )


def incoming_product(left_half, right_half):
    left_cols, right_cols = (
        lax.all_to_all(left_half, "row", split_axis=2, concat_axis=1, tiled=True),
        lax.all_to_all(right_half, "row", split_axis=2, concat_axis=1, tiled=True),
    )
    return lax.dot_general(
        left_cols,
        lax.all_gather(right_cols, "row", axis=2, tiled=True),
        (((1,), (1,)), ((0,), (0,))),
        preferred_element_type=jnp.float32,
    )


def triangle_update(pair_rep, gain_vec, proj_w, out_gain, out_w, pair_mask, incoming):
    normed = normalize(pair_rep.astype(jnp.float32), gain_vec, 2).astype(jnp.bfloat16)
    channels = jnp.einsum(
        "ijd,de->eij", normed, proj_w[:, : 4 * HID], preferred_element_type=jnp.float32
    )
    gate_lin = jnp.einsum(
        "ijd,de->ije", normed, proj_w[:, 4 * HID :], preferred_element_type=jnp.float32
    )
    masked = pair_mask[None, :, :]
    left_proj = (masked * jax.nn.sigmoid(channels[HID : 2 * HID]) * channels[:HID]).astype(
        jnp.bfloat16
    )
    right_proj = (
        masked * jax.nn.sigmoid(channels[3 * HID : 4 * HID]) * channels[2 * HID : 3 * HID]
    ).astype(jnp.bfloat16)
    left_half, right_half = (
        lax.all_to_all(left_proj, "col", split_axis=0, concat_axis=2, tiled=True),
        lax.all_to_all(right_proj, "col", split_axis=0, concat_axis=2, tiled=True),
    )
    if incoming:
        product = incoming_product(left_half, right_half)
    else:
        product = outgoing_product(left_half, right_half)
    mixed = product.astype(jnp.bfloat16)
    mixed_tile = lax.all_to_all(mixed, "col", split_axis=2, concat_axis=0, tiled=True)
    mixed_norm = normalize(mixed_tile.astype(jnp.float32), out_gain[:, None, None], 0).astype(
        jnp.bfloat16
    )
    update = jnp.einsum("cij,cd->ijd", mixed_norm, out_w, preferred_element_type=jnp.float32)
    return (pair_rep.astype(jnp.float32) + jax.nn.sigmoid(gate_lin) * update).astype(jnp.bfloat16)


def local(
    pair_rep,
    residue_mask,
    crop_length,
    norm_gain,
    mult_proj,
    mixed_gain,
    mult_out,
    att_gain,
    att_proj,
    att_bias,
    att_out,
):
    row_count = pair_rep.shape[0]
    col_count = pair_rep.shape[1]
    row_start = lax.axis_index("row") * row_count
    col_start = lax.axis_index("col") * col_count
    positions = jnp.arange(residue_mask.shape[0], dtype=jnp.int32)
    alive = (((residue_mask == 1) | (positions == 0)) & (positions < crop_length[0])).astype(
        jnp.float32
    )
    row_alive = lax.dynamic_slice_in_dim(alive, row_start, row_count, 0)
    col_alive = lax.dynamic_slice_in_dim(alive, col_start, col_count, 0)
    pair_mask = row_alive[:, None] * col_alive[None, :]
    first = triangle_update(
        pair_rep, norm_gain[0], mult_proj[0], mixed_gain[0], mult_out[0], pair_mask, False
    )
    second = triangle_update(
        first, norm_gain[1], mult_proj[1], mixed_gain[1], mult_out[1], pair_mask, True
    )
    normed = normalize(second.astype(jnp.float32), att_gain, 2).astype(jnp.bfloat16)
    projected = jnp.einsum("ijd,de->ije", normed, att_proj, preferred_element_type=jnp.float32)
    queries = projected[..., :ATT].astype(jnp.bfloat16)
    key_rows = projected[..., ATT : 2 * ATT].astype(jnp.bfloat16)
    value_rows = projected[..., 2 * ATT : 3 * ATT].astype(jnp.bfloat16)
    gates = projected[..., 3 * ATT :].astype(jnp.bfloat16)
    bias_tile = jnp.einsum(
        "ijd,dh->hij", normed, att_bias, preferred_element_type=jnp.float32
    ).astype(jnp.bfloat16)
    key_all, value_all, bias_cols = (
        lax.all_gather(key_rows, "col", axis=1, tiled=True),
        lax.all_gather(value_rows, "col", axis=1, tiled=True),
        lax.all_gather(bias_tile, "col", axis=2, tiled=True),
    )
    bias_full = lax.all_gather(bias_cols, "row", axis=1, tiled=True)
    bias_mine = lax.dynamic_slice_in_dim(bias_full, col_start, col_count, 1).astype(jnp.float32)
    total = key_all.shape[1]
    key_mask = jnp.where(alive > 0, 0.0, -1000000000.0).astype(jnp.float32)
    scaling = 1.0 / float(HEAD_DIM) ** 0.5
    query_heads = queries.reshape(row_count, col_count, HEADS, HEAD_DIM)
    key_heads = key_all.reshape(row_count, total, HEADS, HEAD_DIM)
    value_heads = value_all.reshape(row_count, total, HEADS, HEAD_DIM)
    scores = jnp.einsum(
        "ijhd,ikhd->hijk", query_heads, key_heads, preferred_element_type=jnp.float32
    )
    scores = scores * scaling + bias_mine[:, None, :, :] + key_mask[None, None, None, :]
    weights = jax.nn.softmax(scores, axis=-1).astype(jnp.bfloat16)
    attended = jnp.einsum(
        "hijk,ikhd->ijhd", weights, value_heads, preferred_element_type=jnp.float32
    )
    attended = attended.reshape(row_count, col_count, ATT)
    gated = (jax.nn.sigmoid(gates.astype(jnp.float32)) * attended).astype(jnp.bfloat16)
    result = jnp.einsum("ija,ad->ijd", gated, att_out, preferred_element_type=jnp.float32)
    return (second.astype(jnp.float32) + result).astype(jnp.bfloat16)


MESH = pl.DeviceIdType.MESH
BF16 = jnp.bfloat16
F32 = jnp.float32
GROUP = 8
PARTS = 1


def sigmoid(x):
    return 0.5 * jnp.tanh(0.5 * x) + 0.5


def normalize_t(values, gain_col):
    average = jnp.mean(values, axis=0, keepdims=True)
    centered = values - average
    variance = jnp.mean(centered * centered, axis=0, keepdims=True)
    return centered * lax.rsqrt(variance + EPSILON) * gain_col


def mm(a, b, dims=((1,), (0,))):
    return lax.dot_general(a, b, (dims, ((), ())), preferred_element_type=F32)


def fused_kernel(
    n,
    pair_hbm,
    mask_hbm,
    crop_ref,
    gain_hbm,
    proj_hbm,
    mgain_hbm,
    mout_hbm,
    again_hbm,
    aproj_hbm,
    abias_hbm,
    aout_hbm,
    out_ref,
    pair_ref,
    mask_ref,
    gain_ref,
    proj_ref,
    mgain_ref,
    mout_ref,
    again_ref,
    aproj_ref,
    abias_ref,
    aout_ref,
    load_sem,
    zt,
    og,
    f_left,
    f_right,
    fx_left,
    fx_right,
    f_prod,
    f_bias,
    b_pad,
    b_full,
    kmat,
    qvg,
    proj_t,
    out_t,
    gain_cols,
    qvg_t,
    send_lr,
    recv_lr,
    send_p,
    recv_p,
    send_b,
    recv_b,
    send_sem,
    recv_sem,
):
    me = lax.axis_index("row")
    rows, cols, chans = pair_ref.shape
    mine = chans // n
    block = rows * mine
    half = rows // PARTS
    hblock = half * mine
    heads = abias_ref.shape[0]
    att = chans
    hid = chans

    barrier = pltpu.get_barrier_semaphore()
    for s in range(1, n):
        pl.semaphore_signal(
            barrier, inc=1, device_id={"row": lax.rem(me + s, n)}, device_id_type=MESH
        )

    loads = [
        pltpu.make_async_copy(src, dst, load_sem.at[at])
        for at, (src, dst) in enumerate((
            (mask_hbm, mask_ref),
            (gain_hbm, gain_ref),
            (proj_hbm.at[0], proj_ref.at[0]),
            (pair_hbm, pair_ref),
            (mgain_hbm, mgain_ref),
            (proj_hbm.at[1], proj_ref.at[1]),
            (mout_hbm, mout_ref),
            (again_hbm, again_ref),
            (aproj_hbm, aproj_ref),
            (abias_hbm, abias_ref),
            (aout_hbm, aout_ref),
        ))
    ]
    for load in loads:
        load.start()
    rows, cols, chans = pair_ref.shape
    for load in loads[:4]:
        load.wait()

    def column(row_vec):
        return jnp.transpose(jnp.broadcast_to(row_vec.astype(F32), (chans, row_vec.shape[-1])))

    def flip(mat):
        return jnp.transpose(mat.astype(F32)).astype(BF16)

    lane = lax.broadcasted_iota(jnp.int32, (1, cols), 1)
    alive = jnp.where(
        ((mask_ref[...] == 1) | (lane == 0)) & (lane < crop_ref[0]), 1.0, 0.0
    ).astype(F32)

    def row_mask(i):
        here = jnp.where(lane == me * rows + i, alive, 0.0)
        return jnp.sum(here, axis=1, keepdims=True) * alive

    masks = [row_mask(i) for i in range(rows)]

    def exchange(phase, src, dst, p, slot):
        return pltpu.make_async_remote_copy(
            src_ref=src.at[p],
            dst_ref=dst.at[slot],
            send_sem=send_sem.at[phase, p],
            recv_sem=recv_sem.at[phase, slot],
            device_id={"row": p},
            device_id_type=MESH,
        )

    def send_all(phase, src, dst):
        for s in range(n - 1, 0, -1):
            exchange(phase, src, dst, lax.rem(me + s, n), me).start()

    def take_all(phase, src, dst):
        for s in range(1, n):
            q = lax.rem(me + n - s, n)
            exchange(phase, src, dst, q, q).wait_recv()

    def at_row(i):
        return slice(i * cols, (i + 1) * cols)

    def lr_phase(u, k):
        return u * 2 * PARTS + k

    def p_phase(u, k):
        return u * 2 * PARTS + PARTS + k

    def b_phase(k):
        return 4 * PARTS + k

    def project(u, k):
        for i in range(k * half, (k + 1) * half):
            normed = normalize_t(zt[:, at_row(i)].astype(F32), gain_cols[u]).astype(BF16)
            pr = mm(proj_t[u], normed)
            left = masks[i] * sigmoid(pr[hid : 2 * hid]) * pr[:hid]
            right = masks[i] * sigmoid(pr[3 * hid : 4 * hid]) * pr[2 * hid : 3 * hid]
            f_left[:, i] = left.reshape(n, mine, cols)
            f_right[:, i] = right.reshape(n, mine, cols)
            og[:, at_row(i)] = sigmoid(pr[4 * hid :])
        src, dst = send_lr.at[u, k], recv_lr.at[u, k]
        for p in range(n):
            at = slice(k * half, (k + 1) * half)
            src[p, 0] = f_left[p, at].reshape(hblock, cols).astype(BF16)
            src[p, 1] = f_right[p, at].reshape(hblock, cols).astype(BF16)
        if u == 0 and k == 0:
            pl.semaphore_wait(barrier, n - 1)
        send_all(lr_phase(u, k), src, dst)
        dst[me] = src[me]

    def multiply(u):
        for k in range(PARTS):
            src, dst = send_lr.at[u, k], recv_lr.at[u, k]
            take_all(lr_phase(u, k), src, dst)
            for q in range(n):
                at = pl.ds(q * block + k * hblock, hblock)
                fx_left[at, :] = dst[q, 0].astype(F32)
                fx_right[at, :] = dst[q, 1].astype(F32)
        for c in range(mine):
            at = pl.ds(c, n * rows, stride=mine)
            a = fx_left[at, :].astype(BF16)
            b = fx_right[at, :].astype(BF16)
            if u == 0:
                f_prod[at, :] = mm(a, b, ((1,), (1,)))
            else:
                f_prod[at, :] = mm(a, b, ((0,), (0,)))
        for k in range(PARTS):
            src, dst = send_p.at[u, k], recv_p.at[u, k]
            for p in range(n):
                src[p] = f_prod[pl.ds(p * block + k * hblock, hblock), :].astype(BF16)
            send_all(p_phase(u, k), src, dst)
            dst[me] = src[me]

    def finish(u, k):
        src, dst = send_p.at[u, k], recv_p.at[u, k]
        take_all(p_phase(u, k), src, dst)
        for q in range(n):
            f_left[q, k * half : (k + 1) * half] = dst[q].astype(F32).reshape(half, mine, cols)
        for i in range(k * half, (k + 1) * half):
            at = at_row(i)
            mixed = f_left[:, i].reshape(chans, cols)
            mixed_norm = normalize_t(mixed, gain_cols[2 + u]).astype(BF16)
            zt[:, at] = (zt[:, at].astype(F32) + og[:, at] * mm(out_t[u], mixed_norm)).astype(BF16)

    def bias_copy(k, p, slot):
        return pltpu.make_async_remote_copy(
            src_ref=send_b.at[k],
            dst_ref=recv_b.at[k, slot],
            send_sem=send_sem.at[b_phase(k), p],
            recv_sem=recv_sem.at[b_phase(k), slot],
            device_id={"row": p},
            device_id_type=MESH,
        )

    def attention_inputs(k):
        normed_rows = []
        for i in range(k * half, (k + 1) * half):
            normed = normalize_t(zt[:, at_row(i)].astype(F32), gain_cols[4]).astype(BF16)
            normed_rows.append(normed)
            bias_row = mm(b_pad[...].astype(BF16), normed)
            for h in range(heads):
                f_bias[k, h * half + i - k * half : h * half + i - k * half + 1, :] = bias_row[h : h + 1, :]
        send_b[k] = f_bias[k].astype(BF16)
        for s in range(1, n):
            bias_copy(k, lax.rem(me + s, n), me).start()
        recv_b[k, me] = f_bias[k].astype(BF16)
        for i in range(k * half, (k + 1) * half):
            normed = normed_rows[i - k * half]
            kmat[i] = mm(flip(normed), aproj_ref[:, att : 2 * att]).astype(BF16)
            qvg[i] = mm(qvg_t[...], normed).astype(BF16)

    gain_cols[0] = column(gain_ref[0:1, :])
    proj_t[0] = flip(proj_ref[0])
    for i in range(rows):
        zt[:, at_row(i)] = flip(pair_ref[i])
    for k in range(PARTS):
        project(0, k)
    for load in loads[4:]:
        load.wait()
    gain_cols[1] = column(gain_ref[1:2, :])
    gain_cols[2] = column(mgain_ref[0:1, :])
    gain_cols[3] = column(mgain_ref[1:2, :])
    gain_cols[4] = column(again_ref[...])
    proj_t[1] = flip(proj_ref[1])
    for u in range(2):
        out_t[u] = flip(mout_ref[u])
    out_t[2] = flip(aout_ref[...])
    qvg_t[:att] = flip(aproj_ref[:, :att])
    qvg_t[att:] = flip(aproj_ref[:, 2 * att :])
    b_pad[...] = jnp.zeros_like(b_pad)
    b_pad[:heads] = abias_ref[...].astype(F32)
    key_mask = column(jnp.where(alive > 0, 0.0, -1000000000.0))
    multiply(0)
    for k in range(PARTS):
        finish(0, k)
        project(1, k)
    multiply(1)
    for k in range(PARTS):
        finish(1, k)
        attention_inputs(k)

    for k in range(PARTS):
        for s in range(1, n):
            q = lax.rem(me + n - s, n)
            bias_copy(k, q, q).wait_recv()
    for h in range(heads):
        pieces = []
        for q in range(n):
            for k in range(PARTS):
                pieces.append(recv_b[k, q].astype(F32)[h * half : (h + 1) * half])
        b_full[h] = jnp.transpose(jnp.concatenate(pieces, axis=0)) + key_mask
    dim = att // heads
    scaling = 1.0 / float(dim) ** 0.5

    def attend(i, carry):
        parts = []
        for h in range(heads):
            ch = slice(h * dim, (h + 1) * dim)
            scores = mm(kmat[i, :, ch], qvg[i, ch, :]) * scaling + b_full[h]
            top = jnp.max(scores, axis=0, keepdims=True)
            e = jnp.exp(scores - top)
            w = (e * (1.0 / jnp.sum(e, axis=0, keepdims=True))).astype(BF16)
            parts.append(mm(qvg[i, att + h * dim : att + (h + 1) * dim, :], w))
        attended = jnp.concatenate(parts, axis=0)
        gated = (sigmoid(qvg[i, 2 * att :, :].astype(F32)) * attended).astype(BF16)
        result = mm(out_t[2], gated)
        at = pl.ds(pl.multiple_of(i * cols, cols), cols)
        out_ref[i] = jnp.transpose(zt[:, at].astype(F32) + result).astype(BF16)
        return carry

    lax.fori_loop(0, rows, attend, 0, unroll=4)

    def drain(s, carry):
        p = lax.rem(me + s, n)
        for k in range(PARTS):
            for u in range(2):
                exchange(lr_phase(u, k), send_lr.at[u, k], recv_lr.at[u, k], p, me).wait_send()
                exchange(p_phase(u, k), send_p.at[u, k], recv_p.at[u, k], p, me).wait_send()
            bias_copy(k, p, me).wait_send()
        return carry

    lax.fori_loop(1, n, drain, 0)


def fused(n, pair_rep, residue_mask, crop_length, norm_gain, mult_proj, mixed_gain, mult_out,
          att_gain, att_proj, att_bias, att_out):
    rows, cols, chans = pair_rep.shape
    heads = att_bias.shape[1]
    mine = chans // n
    block = rows * mine
    hblock = block // PARTS
    vm = pl.BlockSpec(memory_space=pltpu.VMEM)
    hbm = pl.BlockSpec(memory_space=pltpu.HBM)
    big = n * block

    def far(operand):
        return pltpu.with_memory_space_constraint(operand, pltpu.HBM)

    return pl.pallas_call(
        functools.partial(fused_kernel, n),
        out_shape=jax.ShapeDtypeStruct(pair_rep.shape, BF16),
        in_specs=[hbm, hbm, pl.BlockSpec(memory_space=pltpu.SMEM)] + [hbm] * 8,
        out_specs=vm,
        scratch_shapes=[
            pltpu.VMEM(pair_rep.shape, BF16),
            pltpu.VMEM((1, cols), jnp.int32),
            pltpu.VMEM(norm_gain.shape, F32),
            pltpu.VMEM(mult_proj.shape, BF16),
            pltpu.VMEM(mixed_gain.shape, F32),
            pltpu.VMEM(mult_out.shape, BF16),
            pltpu.VMEM((1, chans), F32),
            pltpu.VMEM(att_proj.shape, BF16),
            pltpu.VMEM((heads, chans), BF16),
            pltpu.VMEM(att_out.shape, BF16),
            pltpu.SemaphoreType.DMA((11,)),
            pltpu.VMEM((chans, rows * cols), BF16),
            pltpu.VMEM((chans, rows * cols), F32),
            pltpu.VMEM((n, rows, mine, cols), F32),
            pltpu.VMEM((n, rows, mine, cols), F32),
            pltpu.VMEM((big, cols), F32),
            pltpu.VMEM((big, cols), F32),
            pltpu.VMEM((big, cols), F32),
            pltpu.VMEM((PARTS, heads * rows // PARTS, cols), F32),
            pltpu.VMEM((2 * GROUP, chans), F32),
            pltpu.VMEM((heads, cols, cols), F32),
            pltpu.VMEM((rows, cols, chans), BF16),
            pltpu.VMEM((rows, 3 * chans, cols), BF16),
            pltpu.VMEM((2, mult_proj.shape[2], chans), BF16),
            pltpu.VMEM((3, chans, chans), BF16),
            pltpu.VMEM((5, chans, cols), F32),
            pltpu.VMEM((3 * chans, chans), BF16),
            pltpu.VMEM((2, PARTS, n, 2, hblock, cols), BF16),
            pltpu.VMEM((2, PARTS, n, 2, hblock, cols), BF16),
            pltpu.VMEM((2, PARTS, n, hblock, cols), BF16),
            pltpu.VMEM((2, PARTS, n, hblock, cols), BF16),
            pltpu.VMEM((PARTS, heads * rows // PARTS, cols), BF16),
            pltpu.VMEM((PARTS, n, heads * rows // PARTS, cols), BF16),
            pltpu.SemaphoreType.DMA((5 * PARTS, n)),
            pltpu.SemaphoreType.DMA((5 * PARTS, n)),
        ],
        compiler_params=pltpu.CompilerParams(
            collective_id=0, has_side_effects=True, vmem_limit_bytes=48 * 1024 * 1024
        ),
        name="fused_pair",
    )(
        far(pair_rep),
        far(residue_mask.reshape(1, -1)),
        crop_length,
        far(norm_gain),
        far(mult_proj),
        far(mixed_gain),
        far(mult_out),
        far(att_gain.reshape(1, -1)),
        far(att_proj),
        far(att_bias.T),
        far(att_out),
    )


def choose(mesh):
    n = mesh.shape["row"]

    def body(pair_rep, *rest):
        rows, cols, chans = pair_rep.shape
        fits = (
            mesh.shape["col"] == 1
            and chans == n * GROUP
            and rows == GROUP
            and cols == n * rows
            and cols == chans
        )
        if fits:
            return fused(n, pair_rep, *rest)
        return local(pair_rep, *rest)

    return body


def solution(mesh):
    placed = (
        P(("groups", "row"), "col", None),
        P("groups"),
        P("groups"),
        P(),
        P(),
        P(),
        P(),
        P(),
        P(),
        P(),
        P(),
    )
    return jax.shard_map(
        choose(mesh),
        mesh=mesh,
        in_specs=placed,
        out_specs=P(("groups", "row"), "col", None),
        check_vma=False,
    )
```

```python
import functools

import jax
import jax.numpy as jnp
from jax import lax
from jax.experimental import pallas as pl
from jax.experimental.pallas import tpu as pltpu
from jax.sharding import PartitionSpec as P

HID = 128
HEADS = 4
HEAD_DIM = 32
ATT = 128


EPSILON = 1e-05


def normalize(values, gain_vec, along):
    average = jnp.mean(values, axis=along, keepdims=True)
    centered = values - average
    variance = jnp.mean(centered * centered, axis=along, keepdims=True)
    return centered * lax.rsqrt(variance + EPSILON) * gain_vec


def outgoing_product(left_half, right_half):
    return lax.dot_general(
        left_half,
        lax.all_gather(right_half, "row", axis=1, tiled=True),
        (((2,), (2,)), ((0,), (0,))),
        preferred_element_type=jnp.float32,
    )


def incoming_product(left_half, right_half):
    left_cols, right_cols = (
        lax.all_to_all(left_half, "row", split_axis=2, concat_axis=1, tiled=True),
        lax.all_to_all(right_half, "row", split_axis=2, concat_axis=1, tiled=True),
    )
    return lax.dot_general(
        left_cols,
        lax.all_gather(right_cols, "row", axis=2, tiled=True),
        (((1,), (1,)), ((0,), (0,))),
        preferred_element_type=jnp.float32,
    )


def triangle_update(pair_rep, gain_vec, proj_w, out_gain, out_w, pair_mask, incoming):
    normed = normalize(pair_rep.astype(jnp.float32), gain_vec, 2).astype(jnp.bfloat16)
    channels = jnp.einsum(
        "ijd,de->eij", normed, proj_w[:, : 4 * HID], preferred_element_type=jnp.float32
    )
    gate_lin = jnp.einsum(
        "ijd,de->ije", normed, proj_w[:, 4 * HID :], preferred_element_type=jnp.float32
    )
    masked = pair_mask[None, :, :]
    left_proj = (masked * jax.nn.sigmoid(channels[HID : 2 * HID]) * channels[:HID]).astype(
        jnp.bfloat16
    )
    right_proj = (
        masked * jax.nn.sigmoid(channels[3 * HID : 4 * HID]) * channels[2 * HID : 3 * HID]
    ).astype(jnp.bfloat16)
    left_half, right_half = (
        lax.all_to_all(left_proj, "col", split_axis=0, concat_axis=2, tiled=True),
        lax.all_to_all(right_proj, "col", split_axis=0, concat_axis=2, tiled=True),
    )
    if incoming:
        product = incoming_product(left_half, right_half)
    else:
        product = outgoing_product(left_half, right_half)
    mixed = product.astype(jnp.bfloat16)
    mixed_tile = lax.all_to_all(mixed, "col", split_axis=2, concat_axis=0, tiled=True)
    mixed_norm = normalize(mixed_tile.astype(jnp.float32), out_gain[:, None, None], 0).astype(
        jnp.bfloat16
    )
    update = jnp.einsum("cij,cd->ijd", mixed_norm, out_w, preferred_element_type=jnp.float32)
    return (pair_rep.astype(jnp.float32) + jax.nn.sigmoid(gate_lin) * update).astype(jnp.bfloat16)


def local(
    pair_rep,
    residue_mask,
    crop_length,
    norm_gain,
    mult_proj,
    mixed_gain,
    mult_out,
    att_gain,
    att_proj,
    att_bias,
    att_out,
):
    row_count = pair_rep.shape[0]
    col_count = pair_rep.shape[1]
    row_start = lax.axis_index("row") * row_count
    col_start = lax.axis_index("col") * col_count
    positions = jnp.arange(residue_mask.shape[0], dtype=jnp.int32)
    alive = (((residue_mask == 1) | (positions == 0)) & (positions < crop_length[0])).astype(
        jnp.float32
    )
    row_alive = lax.dynamic_slice_in_dim(alive, row_start, row_count, 0)
    col_alive = lax.dynamic_slice_in_dim(alive, col_start, col_count, 0)
    pair_mask = row_alive[:, None] * col_alive[None, :]
    first = triangle_update(
        pair_rep, norm_gain[0], mult_proj[0], mixed_gain[0], mult_out[0], pair_mask, False
    )
    second = triangle_update(
        first, norm_gain[1], mult_proj[1], mixed_gain[1], mult_out[1], pair_mask, True
    )
    normed = normalize(second.astype(jnp.float32), att_gain, 2).astype(jnp.bfloat16)
    projected = jnp.einsum("ijd,de->ije", normed, att_proj, preferred_element_type=jnp.float32)
    queries = projected[..., :ATT].astype(jnp.bfloat16)
    key_rows = projected[..., ATT : 2 * ATT].astype(jnp.bfloat16)
    value_rows = projected[..., 2 * ATT : 3 * ATT].astype(jnp.bfloat16)
    gates = projected[..., 3 * ATT :].astype(jnp.bfloat16)
    bias_tile = jnp.einsum(
        "ijd,dh->hij", normed, att_bias, preferred_element_type=jnp.float32
    ).astype(jnp.bfloat16)
    key_all, value_all, bias_cols = (
        lax.all_gather(key_rows, "col", axis=1, tiled=True),
        lax.all_gather(value_rows, "col", axis=1, tiled=True),
        lax.all_gather(bias_tile, "col", axis=2, tiled=True),
    )
    bias_full = lax.all_gather(bias_cols, "row", axis=1, tiled=True)
    bias_mine = lax.dynamic_slice_in_dim(bias_full, col_start, col_count, 1).astype(jnp.float32)
    total = key_all.shape[1]
    key_mask = jnp.where(alive > 0, 0.0, -1000000000.0).astype(jnp.float32)
    scaling = 1.0 / float(HEAD_DIM) ** 0.5
    query_heads = queries.reshape(row_count, col_count, HEADS, HEAD_DIM)
    key_heads = key_all.reshape(row_count, total, HEADS, HEAD_DIM)
    value_heads = value_all.reshape(row_count, total, HEADS, HEAD_DIM)
    scores = jnp.einsum(
        "ijhd,ikhd->hijk", query_heads, key_heads, preferred_element_type=jnp.float32
    )
    scores = scores * scaling + bias_mine[:, None, :, :] + key_mask[None, None, None, :]
    weights = jax.nn.softmax(scores, axis=-1).astype(jnp.bfloat16)
    attended = jnp.einsum(
        "hijk,ikhd->ijhd", weights, value_heads, preferred_element_type=jnp.float32
    )
    attended = attended.reshape(row_count, col_count, ATT)
    gated = (jax.nn.sigmoid(gates.astype(jnp.float32)) * attended).astype(jnp.bfloat16)
    result = jnp.einsum("ija,ad->ijd", gated, att_out, preferred_element_type=jnp.float32)
    return (second.astype(jnp.float32) + result).astype(jnp.bfloat16)


MESH = pl.DeviceIdType.MESH
BF16 = jnp.bfloat16
F32 = jnp.float32
GROUP = 8
FIRST = 1
MIDDLE = 4
LAST = 2
LOG2E = 1.4426950408889634


def sigmoid(x):
    return 0.5 * jnp.tanh(0.5 * x) + 0.5


def normalize_t(values, gain_col):
    average = jnp.mean(values, axis=0, keepdims=True)
    centered = values - average
    variance = jnp.mean(centered * centered, axis=0, keepdims=True)
    return centered * lax.rsqrt(variance + EPSILON) * gain_col


def mm(a, b, dims=((1,), (0,))):
    return lax.dot_general(a, b, (dims, ((), ())), preferred_element_type=F32)


def fused_kernel(
    n,
    pair_hbm,
    mask_hbm,
    crop_ref,
    gain_hbm,
    proj_hbm,
    mgain_hbm,
    mout_hbm,
    again_hbm,
    aproj_hbm,
    abias_hbm,
    aout_hbm,
    out_ref,
    pair_ref,
    mask_ref,
    gain_ref,
    proj_ref,
    mgain_ref,
    mout_ref,
    again_ref,
    aproj_ref,
    abias_ref,
    aout_ref,
    load_sem,
    zt,
    og,
    fx_left,
    fx_right,
    f_prod,
    b_pad,
    b_full,
    kmat,
    q_heads,
    vmat,
    gmat,
    scores,
    proj_t,
    out_t,
    gain_cols,
    qvg_t,
    send_a,
    recv_a,
    send_b,
    recv_b,
    send_c,
    recv_c,
    send_d,
    recv_d,
    send_e,
    recv_e,
    send_sem,
    recv_sem,
):
    me = lax.axis_index("row")
    rows, cols, chans = pair_ref.shape
    peers = n // 2
    mine = chans // n
    wide = chans // peers
    heads = abias_ref.shape[0]
    att = chans
    hid = chans
    dim = att // heads
    here = lax.rem(me, peers)
    near = me - here
    far = peers - near

    barrier = pltpu.get_barrier_semaphore()
    for s in range(1, n):
        pl.semaphore_signal(
            barrier, inc=1, device_id={"row": lax.rem(me + s, n)}, device_id_type=MESH
        )

    loads = [
        pltpu.make_async_copy(src, dst, load_sem.at[at])
        for at, (src, dst) in enumerate((
            (mask_hbm, mask_ref),
            (gain_hbm, gain_ref),
            (proj_hbm.at[0], proj_ref.at[0]),
            (pair_hbm, pair_ref),
            (mgain_hbm, mgain_ref),
            (proj_hbm.at[1], proj_ref.at[1]),
            (mout_hbm, mout_ref),
            (again_hbm, again_ref),
            (aproj_hbm, aproj_ref),
            (abias_hbm, abias_ref),
            (aout_hbm, aout_ref),
        ))
    ]
    for load in loads:
        load.start()
    for load in loads[:4]:
        load.wait()

    def column(row_vec):
        return jnp.transpose(jnp.broadcast_to(row_vec.astype(F32), (chans, row_vec.shape[-1])))

    def flip(mat):
        return jnp.transpose(mat.astype(F32)).astype(BF16)

    lane = lax.broadcasted_iota(jnp.int32, (1, cols), 1)
    alive = jnp.where(
        ((mask_ref[...] == 1) | (lane == 0)) & (lane < crop_ref[0]), 1.0, 0.0
    ).astype(F32)

    def row_mask(i):
        own = jnp.where(lane == me * rows + i, alive, 0.0)
        return jnp.sum(own, axis=1, keepdims=True) * alive

    masks = [row_mask(i) for i in range(rows)]

    def at_row(i):
        return slice(i * cols, (i + 1) * cols)

    def chunk(k, parts):
        return range(k * rows // parts, (k + 1) * rows // parts)

    def remote(phase, src, dst, p):
        return pltpu.make_async_remote_copy(
            src_ref=src,
            dst_ref=dst,
            send_sem=send_sem.at[phase],
            recv_sem=recv_sem.at[phase],
            device_id={"row": p},
            device_id_type=MESH,
        )

    def others():
        return [lax.rem(me + s, n) for s in range(n - 1, 0, -1)]

    def near_others():
        return [near + lax.rem(here + s, peers) for s in range(peers - 1, 0, -1)]

    def far_others():
        return [far + lax.rem(here + s, peers) for s in range(peers - 1, -1, -1)]

    def a_both(k, p):
        src = send_a.at[k, pl.ds(2 * lax.rem(p, peers), 2)]
        return remote(k, src, recv_a.at[k, pl.ds(2 * me, 2)], p)

    def a_right(k, p):
        return remote(k, send_a.at[k, 2 * lax.rem(p, peers) + 1], recv_a.at[k, 2 * me + 1], p)

    def a_all(k):
        block = recv_a.at[k, : 2 * (peers - 1) + peers]
        return remote(k, block, block, me)

    def b_copy(k, p):
        return remote(FIRST + k, send_b.at[k, lax.rem(p, peers)], recv_b.at[k, here], p)

    def b_all(k):
        return remote(FIRST + k, send_b.at[k, : peers - 1], recv_b.at[k, : peers - 1], me)

    def c_copy(k, p):
        return remote(FIRST + MIDDLE + k, send_c.at[k, p], recv_c.at[k, me], p)

    def c_all(k):
        return remote(FIRST + MIDDLE + k, send_c.at[k, : n - 1], recv_c.at[k, : n - 1], me)

    def d_copy(k, p):
        return remote(FIRST + 2 * MIDDLE + k, send_d.at[k, p], recv_d.at[k, me], p)

    def d_all(k):
        return remote(FIRST + 2 * MIDDLE + k, send_d.at[k, : n - 1], recv_d.at[k, : n - 1], me)

    def e_copy(k, p):
        return remote(FIRST + 2 * MIDDLE + LAST + k, send_e.at[k], recv_e.at[k, me], p)

    def e_all(k):
        block = recv_e.at[k, : n - 1]
        return remote(FIRST + 2 * MIDDLE + LAST + k, block, block, me)

    def project(u, i):
        normed = normalize_t(zt[:, at_row(i)].astype(F32), gain_cols[u]).astype(BF16)
        pr = mm(proj_t[u], normed)
        left = masks[i] * sigmoid(pr[hid : 2 * hid]) * pr[:hid]
        right = masks[i] * sigmoid(pr[3 * hid : 4 * hid]) * pr[2 * hid : 3 * hid]
        og[:, at_row(i)] = sigmoid(pr[4 * hid :])
        return left, right

    def start_first(k):
        for r, i in enumerate(chunk(k, FIRST)):
            for side, half in enumerate(project(0, i)):
                parts = half.astype(BF16)
                for p in range(peers):
                    send_a[k, 2 * p + side, r * wide : (r + 1) * wide] = parts[
                        p * wide : (p + 1) * wide
                    ]
        if k == 0:
            pl.semaphore_wait(barrier, n - 1)
        for p in far_others():
            a_right(k, p).start()
        for p in near_others():
            a_both(k, p).start()
        recv_a[k, pl.ds(2 * me, 2)] = send_a[k, pl.ds(2 * here, 2)]

    def multiply_first():
        span = rows // FIRST * wide
        for k in range(FIRST):
            a_all(k).wait_recv()
            for q in range(peers):
                at = q * rows * wide + k * span
                fx_left[at : at + span] = recv_a[k, 2 * (near + q)].astype(F32)
            for q in range(n):
                at = q * rows * wide + k * span
                fx_right[at : at + span] = recv_a[k, 2 * q + 1].astype(F32)
        for c in range(wide):
            at = pl.ds(c, peers * rows, stride=wide)
            a = fx_left[at, :].astype(BF16)
            b = fx_right[pl.ds(c, n * rows, stride=wide), :].astype(BF16)
            f_prod[at, :] = mm(a, b, ((1,), (1,)))
        span = rows // MIDDLE * wide
        for k in range(MIDDLE):
            for p in range(peers):
                send_b[k, p] = f_prod[pl.ds(p * rows * wide + k * span, span), :].astype(BF16)
            for p in near_others():
                b_copy(k, p).start()
            recv_b[k, here] = send_b[k, here]

    def finish(u, i, mixed):
        at = at_row(i)
        mixed_norm = normalize_t(mixed, gain_cols[2 + u]).astype(BF16)
        zt[:, at] = (zt[:, at].astype(F32) + og[:, at] * mm(out_t[u], mixed_norm)).astype(BF16)

    def turn(k):
        b_all(k).wait_recv()
        halves = ([], [])
        for r, i in enumerate(chunk(k, MIDDLE)):
            mixed = recv_b[k, :, r * wide : (r + 1) * wide].reshape(chans, cols).astype(F32)
            finish(0, i, mixed)
            for side, half in enumerate(project(1, i)):
                halves[side].append(half.reshape(n, mine, cols))
        for side in range(2):
            send_c[k, :, side] = jnp.concatenate(halves[side], axis=1).astype(BF16)
        for p in others():
            c_copy(k, p).start()
        recv_c[k, me] = send_c[k, me]

    def multiply_second():
        span = rows // MIDDLE * mine
        for k in range(MIDDLE):
            c_all(k).wait_recv()
            for q in range(n):
                at = q * rows * mine + k * span
                fx_left[at : at + span] = recv_c[k, q, 0].astype(F32)
                fx_right[at : at + span] = recv_c[k, q, 1].astype(F32)
        for c in range(mine):
            at = pl.ds(c, n * rows, stride=mine)
            a = fx_left[at, :].astype(BF16)
            b = fx_right[at, :].astype(BF16)
            f_prod[at, :] = mm(a, b, ((0,), (0,)))
        span = rows // LAST * mine
        for k in range(LAST):
            for p in range(n):
                send_d[k, p] = f_prod[pl.ds(p * rows * mine + k * span, span), :].astype(BF16)
            for p in others():
                d_copy(k, p).start()
            recv_d[k, me] = send_d[k, me]

    def close(k):
        d_all(k).wait_recv()
        mixed_all = recv_d[k].astype(F32)
        biases = []
        normed_rows = []
        for r, i in enumerate(chunk(k, LAST)):
            finish(1, i, mixed_all[:, r * mine : (r + 1) * mine].reshape(chans, cols))
            normed = normalize_t(zt[:, at_row(i)].astype(F32), gain_cols[4]).astype(BF16)
            normed_rows.append(normed)
            biases.append(mm(b_pad[...].astype(BF16), normed))
        send_e[k] = jnp.concatenate(
            [row[h : h + 1] for h in range(heads) for row in biases], axis=0
        ).astype(BF16)
        for p in others():
            e_copy(k, p).start()
        recv_e[k, me] = send_e[k]
        return normed_rows

    def attention_inputs(k, normed_rows):
        for i, normed in zip(chunk(k, LAST), normed_rows):
            kmat[i] = mm(flip(normed), aproj_ref[:, att : 2 * att]).astype(BF16)
            qvg = mm(qvg_t[...], normed).astype(BF16)
            for h in range(heads):
                ch = slice(h * dim, (h + 1) * dim)
                q_heads[i, ch, h * cols : (h + 1) * cols] = qvg[ch]
            vmat[i] = qvg[att : 2 * att]
            gmat[i] = sigmoid(qvg[2 * att :].astype(F32))
            scores[i] = mm(kmat[i], q_heads[i]) * (LOG2E / float(dim) ** 0.5)

    gain_cols[0] = column(gain_ref[0:1, :])
    proj_t[0] = flip(proj_ref[0])
    for i in range(rows):
        zt[:, at_row(i)] = flip(pair_ref[i])
    for k in range(FIRST):
        start_first(k)
    for load in loads[4:]:
        load.wait()
    gain_cols[1] = column(gain_ref[1:2, :])
    gain_cols[2] = column(mgain_ref[0:1, :])
    gain_cols[3] = column(mgain_ref[1:2, :])
    gain_cols[4] = column(again_ref[...])
    proj_t[1] = flip(proj_ref[1])
    for u in range(2):
        out_t[u] = flip(mout_ref[u])
    out_t[2] = flip(aout_ref[...])
    qvg_t[:att] = flip(aproj_ref[:, :att])
    qvg_t[att:] = flip(aproj_ref[:, 2 * att :])
    b_pad[...] = jnp.zeros_like(b_pad)
    b_pad[:heads] = abias_ref[...].astype(F32)
    q_heads[...] = jnp.zeros_like(q_heads)
    key_mask = column(jnp.where(alive > 0, 0.0, -1000000000.0))
    multiply_first()
    for k in range(MIDDLE):
        turn(k)
    for k in range(FIRST):
        a_all(k).wait_send()
    for k in range(MIDDLE):
        b_all(k).wait_send()
    multiply_second()
    for k in range(MIDDLE):
        c_all(k).wait_send()
    closed = [close(k) for k in range(LAST)]
    for k in range(LAST):
        attention_inputs(k, closed[k])
    for k in range(LAST):
        d_all(k).wait_send()

    for k in range(LAST):
        e_all(k).wait_recv()
    part = rows // LAST
    for h in range(heads):
        pieces = []
        for q in range(n):
            for k in range(LAST):
                pieces.append(recv_e[k, q].astype(F32)[h * part : (h + 1) * part])
        across = jnp.transpose(jnp.concatenate(pieces, axis=0))
        b_full[:, h * cols : (h + 1) * cols] = (across + key_mask) * LOG2E

    def attend(i, carry):
        parts = []
        for h in range(heads):
            at = slice(h * cols, (h + 1) * cols)
            total = scores[i, :, at] + b_full[:, at]
            e = jnp.exp2(total - jnp.max(total, axis=0, keepdims=True))
            inverse = 1.0 / jnp.sum(e, axis=0, keepdims=True)
            w = (e * inverse).astype(BF16)
            parts.append(mm(vmat[i, h * dim : (h + 1) * dim, :], w))
        attended = jnp.concatenate(parts, axis=0)
        gated = (gmat[i] * attended).astype(BF16)
        result = mm(out_t[2], gated)
        at = pl.ds(pl.multiple_of(i * cols, cols), cols)
        out_ref[i] = jnp.transpose(zt[:, at].astype(F32) + result).astype(BF16)
        return carry

    lax.fori_loop(0, rows, attend, 0, unroll=4)

    for k in range(LAST):
        e_all(k).wait_send()


def fused(n, pair_rep, residue_mask, crop_length, norm_gain, mult_proj, mixed_gain, mult_out,
          att_gain, att_proj, att_bias, att_out):
    rows, cols, chans = pair_rep.shape
    heads = att_bias.shape[1]
    peers = n // 2
    mine = chans // n
    wide = chans // peers
    vm = pl.BlockSpec(memory_space=pltpu.VMEM)
    hbm = pl.BlockSpec(memory_space=pltpu.HBM)
    phases = FIRST + 2 * MIDDLE + 2 * LAST
    first = pltpu.VMEM((FIRST, 2 * peers, rows // FIRST * wide, cols), BF16)
    first_in = pltpu.VMEM((FIRST, 2 * n, rows // FIRST * wide, cols), BF16)
    back = pltpu.VMEM((MIDDLE, peers, rows // MIDDLE * wide, cols), BF16)
    second = pltpu.VMEM((MIDDLE, n, 2, rows // MIDDLE * mine, cols), BF16)
    home = pltpu.VMEM((LAST, n, rows // LAST * mine, cols), BF16)
    bias = pltpu.VMEM((LAST, heads * rows // LAST, cols), BF16)
    bias_in = pltpu.VMEM((LAST, n, heads * rows // LAST, cols), BF16)

    def far(operand):
        return pltpu.with_memory_space_constraint(operand, pltpu.HBM)

    return pl.pallas_call(
        functools.partial(fused_kernel, n),
        out_shape=jax.ShapeDtypeStruct(pair_rep.shape, BF16),
        in_specs=[hbm, hbm, pl.BlockSpec(memory_space=pltpu.SMEM)] + [hbm] * 8,
        out_specs=vm,
        scratch_shapes=[
            pltpu.VMEM(pair_rep.shape, BF16),
            pltpu.VMEM((1, cols), jnp.int32),
            pltpu.VMEM(norm_gain.shape, F32),
            pltpu.VMEM(mult_proj.shape, BF16),
            pltpu.VMEM(mixed_gain.shape, F32),
            pltpu.VMEM(mult_out.shape, BF16),
            pltpu.VMEM((1, chans), F32),
            pltpu.VMEM(att_proj.shape, BF16),
            pltpu.VMEM((heads, chans), BF16),
            pltpu.VMEM(att_out.shape, BF16),
            pltpu.SemaphoreType.DMA((11,)),
            pltpu.VMEM((chans, rows * cols), BF16),
            pltpu.VMEM((chans, rows * cols), F32),
            pltpu.VMEM((n * rows * mine, cols), F32),
            pltpu.VMEM((n * rows * wide, cols), F32),
            pltpu.VMEM((n * rows * mine, cols), F32),
            pltpu.VMEM((2 * GROUP, chans), F32),
            pltpu.VMEM((cols, heads * cols), F32),
            pltpu.VMEM((rows, cols, chans), BF16),
            pltpu.VMEM((rows, chans, heads * cols), BF16),
            pltpu.VMEM((rows, chans, cols), BF16),
            pltpu.VMEM((rows, chans, cols), F32),
            pltpu.VMEM((rows, cols, heads * cols), F32),
            pltpu.VMEM((2, mult_proj.shape[2], chans), BF16),
            pltpu.VMEM((3, chans, chans), BF16),
            pltpu.VMEM((5, chans, cols), F32),
            pltpu.VMEM((3 * chans, chans), BF16),
            first,
            first_in,
            back,
            back,
            second,
            second,
            home,
            home,
            bias,
            bias_in,
            pltpu.SemaphoreType.DMA((phases,)),
            pltpu.SemaphoreType.DMA((phases,)),
        ],
        compiler_params=pltpu.CompilerParams(
            collective_id=0, has_side_effects=True, vmem_limit_bytes=48 * 1024 * 1024
        ),
        name="fused_pair",
    )(
        far(pair_rep),
        far(residue_mask.reshape(1, -1)),
        crop_length,
        far(norm_gain),
        far(mult_proj),
        far(mixed_gain),
        far(mult_out),
        far(att_gain.reshape(1, -1)),
        far(att_proj),
        far(att_bias.T),
        far(att_out),
    )


def choose(mesh):
    n = mesh.shape["row"]

    def body(pair_rep, *rest):
        rows, cols, chans = pair_rep.shape
        fits = (
            mesh.shape["col"] == 1
            and n % 2 == 0
            and chans == n * GROUP
            and rows == GROUP
            and cols == n * rows
            and cols == chans
        )
        if fits:
            return fused(n, pair_rep, *rest)
        return local(pair_rep, *rest)

    return body


def solution(mesh):
    placed = (
        P(("groups", "row"), "col", None),
        P("groups"),
        P("groups"),
        P(),
        P(),
        P(),
        P(),
        P(),
        P(),
        P(),
        P(),
    )
    return jax.shard_map(
        choose(mesh),
        mesh=mesh,
        in_specs=placed,
        out_specs=P(("groups", "row"), "col", None),
        check_vma=False,
    )
```

```python
import functools

import jax
import jax.numpy as jnp
from jax import lax
from jax.experimental import pallas as pl
from jax.experimental.pallas import tpu as pltpu
from jax.sharding import PartitionSpec as P

HID = 128
HEADS = 4
HEAD_DIM = 32
ATT = 128


EPSILON = 1e-05


def normalize(values, gain_vec, along):
    average = jnp.mean(values, axis=along, keepdims=True)
    centered = values - average
    variance = jnp.mean(centered * centered, axis=along, keepdims=True)
    return centered * lax.rsqrt(variance + EPSILON) * gain_vec


def outgoing_product(left_half, right_half):
    return lax.dot_general(
        left_half,
        lax.all_gather(right_half, "row", axis=1, tiled=True),
        (((2,), (2,)), ((0,), (0,))),
        preferred_element_type=jnp.float32,
    )


def incoming_product(left_half, right_half):
    left_cols, right_cols = (
        lax.all_to_all(left_half, "row", split_axis=2, concat_axis=1, tiled=True),
        lax.all_to_all(right_half, "row", split_axis=2, concat_axis=1, tiled=True),
    )
    return lax.dot_general(
        left_cols,
        lax.all_gather(right_cols, "row", axis=2, tiled=True),
        (((1,), (1,)), ((0,), (0,))),
        preferred_element_type=jnp.float32,
    )


def triangle_update(pair_rep, gain_vec, proj_w, out_gain, out_w, pair_mask, incoming):
    normed = normalize(pair_rep.astype(jnp.float32), gain_vec, 2).astype(jnp.bfloat16)
    channels = jnp.einsum(
        "ijd,de->eij", normed, proj_w[:, : 4 * HID], preferred_element_type=jnp.float32
    )
    gate_lin = jnp.einsum(
        "ijd,de->ije", normed, proj_w[:, 4 * HID :], preferred_element_type=jnp.float32
    )
    masked = pair_mask[None, :, :]
    left_proj = (masked * jax.nn.sigmoid(channels[HID : 2 * HID]) * channels[:HID]).astype(
        jnp.bfloat16
    )
    right_proj = (
        masked * jax.nn.sigmoid(channels[3 * HID : 4 * HID]) * channels[2 * HID : 3 * HID]
    ).astype(jnp.bfloat16)
    left_half, right_half = (
        lax.all_to_all(left_proj, "col", split_axis=0, concat_axis=2, tiled=True),
        lax.all_to_all(right_proj, "col", split_axis=0, concat_axis=2, tiled=True),
    )
    if incoming:
        product = incoming_product(left_half, right_half)
    else:
        product = outgoing_product(left_half, right_half)
    mixed = product.astype(jnp.bfloat16)
    mixed_tile = lax.all_to_all(mixed, "col", split_axis=2, concat_axis=0, tiled=True)
    mixed_norm = normalize(mixed_tile.astype(jnp.float32), out_gain[:, None, None], 0).astype(
        jnp.bfloat16
    )
    update = jnp.einsum("cij,cd->ijd", mixed_norm, out_w, preferred_element_type=jnp.float32)
    return (pair_rep.astype(jnp.float32) + jax.nn.sigmoid(gate_lin) * update).astype(jnp.bfloat16)


def local(
    pair_rep,
    residue_mask,
    crop_length,
    norm_gain,
    mult_proj,
    mixed_gain,
    mult_out,
    att_gain,
    att_proj,
    att_bias,
    att_out,
):
    row_count = pair_rep.shape[0]
    col_count = pair_rep.shape[1]
    row_start = lax.axis_index("row") * row_count
    col_start = lax.axis_index("col") * col_count
    positions = jnp.arange(residue_mask.shape[0], dtype=jnp.int32)
    alive = (((residue_mask == 1) | (positions == 0)) & (positions < crop_length[0])).astype(
        jnp.float32
    )
    row_alive = lax.dynamic_slice_in_dim(alive, row_start, row_count, 0)
    col_alive = lax.dynamic_slice_in_dim(alive, col_start, col_count, 0)
    pair_mask = row_alive[:, None] * col_alive[None, :]
    first = triangle_update(
        pair_rep, norm_gain[0], mult_proj[0], mixed_gain[0], mult_out[0], pair_mask, False
    )
    second = triangle_update(
        first, norm_gain[1], mult_proj[1], mixed_gain[1], mult_out[1], pair_mask, True
    )
    normed = normalize(second.astype(jnp.float32), att_gain, 2).astype(jnp.bfloat16)
    projected = jnp.einsum("ijd,de->ije", normed, att_proj, preferred_element_type=jnp.float32)
    queries = projected[..., :ATT].astype(jnp.bfloat16)
    key_rows = projected[..., ATT : 2 * ATT].astype(jnp.bfloat16)
    value_rows = projected[..., 2 * ATT : 3 * ATT].astype(jnp.bfloat16)
    gates = projected[..., 3 * ATT :].astype(jnp.bfloat16)
    bias_tile = jnp.einsum(
        "ijd,dh->hij", normed, att_bias, preferred_element_type=jnp.float32
    ).astype(jnp.bfloat16)
    key_all, value_all, bias_cols = (
        lax.all_gather(key_rows, "col", axis=1, tiled=True),
        lax.all_gather(value_rows, "col", axis=1, tiled=True),
        lax.all_gather(bias_tile, "col", axis=2, tiled=True),
    )
    bias_full = lax.all_gather(bias_cols, "row", axis=1, tiled=True)
    bias_mine = lax.dynamic_slice_in_dim(bias_full, col_start, col_count, 1).astype(jnp.float32)
    total = key_all.shape[1]
    key_mask = jnp.where(alive > 0, 0.0, -1000000000.0).astype(jnp.float32)
    scaling = 1.0 / float(HEAD_DIM) ** 0.5
    query_heads = queries.reshape(row_count, col_count, HEADS, HEAD_DIM)
    key_heads = key_all.reshape(row_count, total, HEADS, HEAD_DIM)
    value_heads = value_all.reshape(row_count, total, HEADS, HEAD_DIM)
    scores = jnp.einsum(
        "ijhd,ikhd->hijk", query_heads, key_heads, preferred_element_type=jnp.float32
    )
    scores = scores * scaling + bias_mine[:, None, :, :] + key_mask[None, None, None, :]
    weights = jax.nn.softmax(scores, axis=-1).astype(jnp.bfloat16)
    attended = jnp.einsum(
        "hijk,ikhd->ijhd", weights, value_heads, preferred_element_type=jnp.float32
    )
    attended = attended.reshape(row_count, col_count, ATT)
    gated = (jax.nn.sigmoid(gates.astype(jnp.float32)) * attended).astype(jnp.bfloat16)
    result = jnp.einsum("ija,ad->ijd", gated, att_out, preferred_element_type=jnp.float32)
    return (second.astype(jnp.float32) + result).astype(jnp.bfloat16)


MESH = pl.DeviceIdType.MESH
BF16 = jnp.bfloat16
F32 = jnp.float32
GROUP = 8
FIRST = 1
MIDDLE = 4
SHARED = 2
LAST = 2
LOG2E = 1.4426950408889634


def sigmoid(x):
    return 0.5 * jnp.tanh(0.5 * x) + 0.5


def normalize_t(values, gain_col):
    average = jnp.mean(values, axis=0, keepdims=True)
    centered = values - average
    variance = jnp.mean(centered * centered, axis=0, keepdims=True)
    return centered * lax.rsqrt(variance + EPSILON) * gain_col


def mm(a, b, dims=((1,), (0,))):
    return lax.dot_general(a, b, (dims, ((), ())), preferred_element_type=F32)


def fused_kernel(
    n,
    pair_hbm,
    mask_hbm,
    crop_ref,
    gain_hbm,
    proj_hbm,
    mgain_hbm,
    mout_hbm,
    again_hbm,
    aproj_hbm,
    abias_hbm,
    aout_hbm,
    out_ref,
    pair_ref,
    mask_ref,
    gain_ref,
    proj_ref,
    mgain_ref,
    mout_ref,
    again_ref,
    aproj_ref,
    abias_ref,
    aout_ref,
    load_sem,
    zt,
    og,
    fx_left,
    fx_right,
    f_prod,
    b_pad,
    b_full,
    kmat,
    q_heads,
    vmat,
    gmat,
    scores,
    proj_t,
    out_t,
    gain_cols,
    qvg_t,
    send_a,
    recv_a,
    send_b,
    recv_b,
    send_c,
    recv_c,
    send_f,
    recv_f,
    send_d,
    recv_d,
    send_g,
    recv_g,
    send_e,
    recv_e,
    send_sem,
    recv_sem,
):
    me = lax.axis_index("row")
    rows, cols, chans = pair_ref.shape
    peers = n // 2
    mine = chans // n
    wide = chans // peers
    heads = abias_ref.shape[0]
    att = chans
    hid = chans
    dim = att // heads
    here = lax.rem(me, peers)
    near = me - here
    far = peers - near

    c_phase = FIRST + MIDDLE
    f_phase = c_phase + MIDDLE
    d_phase = f_phase + SHARED
    g_phase = d_phase + LAST
    e_phase = g_phase + LAST
    few = mine // 2

    barrier = pltpu.get_barrier_semaphore()
    for s in range(1, n):
        pl.semaphore_signal(
            barrier, inc=1, device_id={"row": lax.rem(me + s, n)}, device_id_type=MESH
        )

    loads = [
        pltpu.make_async_copy(src, dst, load_sem.at[at])
        for at, (src, dst) in enumerate((
            (mask_hbm, mask_ref),
            (gain_hbm, gain_ref),
            (proj_hbm.at[0], proj_ref.at[0]),
            (pair_hbm, pair_ref),
            (mgain_hbm, mgain_ref),
            (proj_hbm.at[1], proj_ref.at[1]),
            (mout_hbm, mout_ref),
            (again_hbm, again_ref),
            (aproj_hbm, aproj_ref),
            (abias_hbm, abias_ref),
            (aout_hbm, aout_ref),
        ))
    ]
    for load in loads:
        load.start()
    for load in loads[:4]:
        load.wait()

    def column(row_vec):
        return jnp.transpose(jnp.broadcast_to(row_vec.astype(F32), (chans, row_vec.shape[-1])))

    def flip(mat):
        return jnp.transpose(mat.astype(F32)).astype(BF16)

    lane = lax.broadcasted_iota(jnp.int32, (1, cols), 1)
    alive = jnp.where(
        ((mask_ref[...] == 1) | (lane == 0)) & (lane < crop_ref[0]), 1.0, 0.0
    ).astype(F32)

    def row_mask(i):
        own = jnp.where(lane == me * rows + i, alive, 0.0)
        return jnp.sum(own, axis=1, keepdims=True) * alive

    masks = [row_mask(i) for i in range(rows)]

    def at_row(i):
        return slice(i * cols, (i + 1) * cols)

    def chunk(k, parts):
        return range(k * rows // parts, (k + 1) * rows // parts)

    def remote(phase, src, dst, p):
        return pltpu.make_async_remote_copy(
            src_ref=src,
            dst_ref=dst,
            send_sem=send_sem.at[phase],
            recv_sem=recv_sem.at[phase],
            device_id={"row": p},
            device_id_type=MESH,
        )

    def partner(s):
        place, at = 1, 0
        while place < n:
            bit = lax.rem(lax.div(me, place) + s // place % 2, 2)
            at, place = at + place * bit, 2 * place
        return at

    def others():
        return [partner(s) for s in range(n - 1, 0, -1)]

    def near_others():
        return [partner(s) for s in range(peers - 1, 0, -1)]

    def far_others():
        return [partner(s) for s in range(n - 1, peers - 1, -1)]

    def a_both(k, p):
        src = send_a.at[k, pl.ds(2 * lax.rem(p, peers), 2)]
        return remote(k, src, recv_a.at[k, pl.ds(2 * me, 2)], p)

    def a_right(k, p):
        return remote(k, send_a.at[k, 2 * lax.rem(p, peers) + 1], recv_a.at[k, 2 * me + 1], p)

    def a_all(k):
        block = recv_a.at[k, : 2 * (peers - 1) + peers]
        return remote(k, block, block, me)

    def b_copy(k, p):
        return remote(FIRST + k, send_b.at[k, lax.rem(p, peers)], recv_b.at[k, here], p)

    def b_all(k):
        return remote(FIRST + k, send_b.at[k, : peers - 1], recv_b.at[k, : peers - 1], me)

    def c_copy(k, p):
        return remote(c_phase + k, send_c.at[k, lax.rem(p, peers)], recv_c.at[k, here], p)

    def c_all(k):
        return remote(c_phase + k, send_c.at[k, : peers - 1], recv_c.at[k, : peers - 1], me)

    def f_copy(k, p):
        return remote(f_phase + k, send_f.at[k, p], recv_f.at[k, me], p)

    def f_all(k):
        return remote(f_phase + k, send_f.at[k, : n - 1], recv_f.at[k, : n - 1], me)

    def d_copy(k, p):
        return remote(d_phase + k, send_d.at[k, p], recv_d.at[k, me], p)

    def d_all(k):
        return remote(d_phase + k, send_d.at[k, : n - 1], recv_d.at[k, : n - 1], me)

    def g_copy(k, p):
        return remote(g_phase + k, send_g.at[k, p], recv_g.at[k, me], p)

    def g_all(k):
        return remote(g_phase + k, send_g.at[k, : n - 1], recv_g.at[k, : n - 1], me)

    def e_copy(k, p):
        return remote(e_phase + k, send_e.at[k], recv_e.at[k, me], p)

    def e_all(k):
        block = recv_e.at[k, : n - 1]
        return remote(e_phase + k, block, block, me)

    def project(u, i):
        normed = normalize_t(zt[:, at_row(i)].astype(F32), gain_cols[u]).astype(BF16)
        pr = mm(proj_t[u], normed)
        left = masks[i] * sigmoid(pr[hid : 2 * hid]) * pr[:hid]
        right = masks[i] * sigmoid(pr[3 * hid : 4 * hid]) * pr[2 * hid : 3 * hid]
        og[:, at_row(i)] = sigmoid(pr[4 * hid :])
        return left, right

    def start_first(k):
        for r, i in enumerate(chunk(k, FIRST)):
            for side, half in enumerate(project(0, i)):
                parts = half.astype(BF16)
                for p in range(peers):
                    send_a[k, 2 * p + side, r * wide : (r + 1) * wide] = parts[
                        p * wide : (p + 1) * wide
                    ]
        if k == 0:
            pl.semaphore_wait(barrier, n - 1)
        for p in far_others():
            a_right(k, p).start()
        for p in near_others():
            a_both(k, p).start()
        recv_a[k, pl.ds(2 * me, 2)] = send_a[k, pl.ds(2 * here, 2)]

    def multiply_first():
        span = rows // FIRST * wide
        for k in range(FIRST):
            a_all(k).wait_recv()
            for q in range(peers):
                at = q * rows * wide + k * span
                fx_left[at : at + span] = recv_a[k, 2 * (near + q)].astype(F32)
            for q in range(n):
                at = q * rows * wide + k * span
                fx_right[at : at + span] = recv_a[k, 2 * q + 1].astype(F32)
        for c in range(wide):
            at = pl.ds(c, peers * rows, stride=wide)
            a = fx_left[at, :].astype(BF16)
            b = fx_right[pl.ds(c, n * rows, stride=wide), :].astype(BF16)
            f_prod[at, :] = mm(a, b, ((1,), (1,)))
        span = rows // MIDDLE * wide
        for k in range(MIDDLE):
            for p in range(peers):
                send_b[k, p] = f_prod[pl.ds(p * rows * wide + k * span, span), :].astype(BF16)
            for p in near_others():
                b_copy(k, p).start()
            recv_b[k, here] = send_b[k, here]

    def finish(u, i, mixed):
        at = at_row(i)
        mixed_norm = normalize_t(mixed, gain_cols[2 + u]).astype(BF16)
        zt[:, at] = (zt[:, at].astype(F32) + og[:, at] * mm(out_t[u], mixed_norm)).astype(BF16)

    low = lax.broadcasted_iota(jnp.int32, (peers * mine, cols), 0) % mine < few

    def trade(x, y):
        x, y = x.reshape(peers * mine, cols), y.reshape(peers * mine, cols)
        up = pltpu.roll(x, peers * mine - few, 0)
        down = pltpu.roll(y, few, 0)
        pair = jnp.where(low, x, down), jnp.where(low, up, y)
        return [half.reshape(peers, mine, cols) for half in pair]

    shared = (([], []), ([], []))

    def turn(k):
        b_all(k).wait_recv()
        halves = ([], [])
        for r, i in enumerate(chunk(k, MIDDLE)):
            mixed = recv_b[k, :, r * wide : (r + 1) * wide].reshape(chans, cols).astype(F32)
            finish(0, i, mixed)
            for side, half in enumerate(project(1, i)):
                halves[side].append(half.reshape(peers, 2, mine, cols))
        for side in range(2):
            block = jnp.concatenate([half[:, 0] for half in halves[side]], axis=1)
            send_c[k, :, side] = block.astype(BF16)
            for r in range(0, rows // MIDDLE, 2):
                upper, lower = halves[side][r][:, 1], halves[side][r + 1][:, 1]
                for to, pair in enumerate(trade(upper, lower)):
                    shared[side][to].append(pair)
        for p in near_others():
            c_copy(k, p).start()
        recv_c[k, here] = send_c[k, here]
        if (k + 1) % (MIDDLE // SHARED) == 0:
            at = k * SHARED // MIDDLE
            for side in range(2):
                for to in range(2):
                    block = jnp.concatenate(shared[side][to], axis=1)
                    send_f[at, to * peers : (to + 1) * peers, side] = block.astype(BF16)
                    shared[side][to].clear()
            recv_f[at, me] = send_f[at, me]

    def partial_products():
        span = rows // MIDDLE * mine
        for k in range(MIDDLE):
            c_all(k).wait_recv()
            for q in range(peers):
                at = q * rows * mine + k * span
                fx_left[at : at + span] = recv_c[k, q, 0].astype(F32)
                fx_right[at : at + span] = recv_c[k, q, 1].astype(F32)
        for c in range(mine):
            at = pl.ds(c, peers * rows, stride=mine)
            a = fx_left[at, :].astype(BF16)
            b = fx_right[at, :].astype(BF16)
            f_prod[pl.ds(c, n * rows, stride=mine), :] = mm(a, b, ((0,), (0,)))
        span = rows // LAST * mine
        for k in range(LAST):
            for p in range(n):
                send_d[k, p] = f_prod[pl.ds(p * rows * mine + k * span, span), :].astype(BF16)
            recv_d[k, me] = send_d[k, me]
            if k == 0:
                for p in others():
                    d_copy(k, p).start()

    def shared_products():
        span = rows // SHARED * few
        for k in range(SHARED):
            f_all(k).wait_recv()
            for q in range(n):
                at = q * rows * few + k * span
                fx_left[at : at + span] = recv_f[k, q, 0].astype(F32)
                fx_right[at : at + span] = recv_f[k, q, 1].astype(F32)
        for c in range(few):
            at = pl.ds(c, n * rows, stride=few)
            a = fx_left[at, :].astype(BF16)
            b = fx_right[at, :].astype(BF16)
            f_prod[at, :] = mm(a, b, ((0,), (0,)))
        span = rows // LAST * few
        for k in range(LAST):
            for p in range(n):
                send_g[k, p] = f_prod[pl.ds(p * rows * few + k * span, span), :].astype(BF16)
            if k > 0:
                for p in others():
                    d_copy(k, p).start()
            for p in others():
                g_copy(k, p).start()
            recv_g[k, me] = send_g[k, me]

    def close(k):
        d_all(k).wait_recv()
        both = recv_d[k].astype(F32)
        summed = both[:peers] + both[peers:]
        g_all(k).wait_recv()
        ends = recv_g[k].astype(F32)
        tails = []
        for r in range(0, rows // LAST, 2):
            pair = ends[:, r * few : (r + 2) * few]
            tails += trade(pair[:peers], pair[peers:])
        biases = []
        normed_rows = []
        for r, i in enumerate(chunk(k, LAST)):
            mixed = jnp.concatenate([summed[:, r * mine : (r + 1) * mine], tails[r]], axis=1)
            finish(1, i, mixed.reshape(chans, cols))
            normed = normalize_t(zt[:, at_row(i)].astype(F32), gain_cols[4]).astype(BF16)
            normed_rows.append(normed)
            biases.append(mm(b_pad[...].astype(BF16), normed))
        send_e[k] = jnp.concatenate(
            [row[h : h + 1] for h in range(heads) for row in biases], axis=0
        ).astype(BF16)
        for p in others():
            e_copy(k, p).start()
        recv_e[k, me] = send_e[k]
        return normed_rows

    def attention_inputs(k, normed_rows):
        for i, normed in zip(chunk(k, LAST), normed_rows):
            kmat[i] = mm(flip(normed), aproj_ref[:, att : 2 * att]).astype(BF16)
            qvg = mm(qvg_t[...], normed).astype(BF16)
            for h in range(heads):
                ch = slice(h * dim, (h + 1) * dim)
                q_heads[i, ch, h * cols : (h + 1) * cols] = qvg[ch]
            vmat[i] = qvg[att : 2 * att]
            gmat[i] = sigmoid(qvg[2 * att :].astype(F32))
            scores[i] = mm(kmat[i], q_heads[i]) * (LOG2E / float(dim) ** 0.5)

    gain_cols[0] = column(gain_ref[0:1, :])
    proj_t[0] = flip(proj_ref[0])
    for i in range(rows):
        zt[:, at_row(i)] = flip(pair_ref[i])
    for k in range(FIRST):
        start_first(k)
    for load in loads[4:]:
        load.wait()
    gain_cols[1] = column(gain_ref[1:2, :])
    gain_cols[2] = column(mgain_ref[0:1, :])
    gain_cols[3] = column(mgain_ref[1:2, :])
    gain_cols[4] = column(again_ref[...])
    proj_t[1] = flip(proj_ref[1])
    for u in range(2):
        out_t[u] = flip(mout_ref[u])
    out_t[2] = flip(aout_ref[...])
    qvg_t[:att] = flip(aproj_ref[:, :att])
    qvg_t[att:] = flip(aproj_ref[:, 2 * att :])
    b_pad[...] = jnp.zeros_like(b_pad)
    b_pad[:heads] = abias_ref[...].astype(F32)
    q_heads[...] = jnp.zeros_like(q_heads)
    key_mask = column(jnp.where(alive > 0, 0.0, -1000000000.0))
    multiply_first()
    for k in range(MIDDLE):
        turn(k)
    for k in range(SHARED):
        for p in others():
            f_copy(k, p).start()
    for k in range(FIRST):
        a_all(k).wait_send()
    for k in range(MIDDLE):
        b_all(k).wait_send()
    partial_products()
    shared_products()
    for k in range(MIDDLE):
        c_all(k).wait_send()
    for k in range(SHARED):
        f_all(k).wait_send()
    for k in range(LAST):
        attention_inputs(k, close(k))
    for k in range(LAST):
        d_all(k).wait_send()
        g_all(k).wait_send()

    for k in range(LAST):
        e_all(k).wait_recv()
    part = rows // LAST
    for h in range(heads):
        pieces = []
        for q in range(n):
            for k in range(LAST):
                pieces.append(recv_e[k, q].astype(F32)[h * part : (h + 1) * part])
        across = jnp.transpose(jnp.concatenate(pieces, axis=0))
        b_full[:, h * cols : (h + 1) * cols] = (across + key_mask) * LOG2E

    def attend(i, carry):
        parts = []
        for h in range(heads):
            at = slice(h * cols, (h + 1) * cols)
            total = scores[i, :, at] + b_full[:, at]
            e = jnp.exp2(total - jnp.max(total, axis=0, keepdims=True))
            inverse = 1.0 / jnp.sum(e, axis=0, keepdims=True)
            w = (e * inverse).astype(BF16)
            parts.append(mm(vmat[i, h * dim : (h + 1) * dim, :], w))
        attended = jnp.concatenate(parts, axis=0)
        gated = (gmat[i] * attended).astype(BF16)
        result = mm(out_t[2], gated)
        at = pl.ds(pl.multiple_of(i * cols, cols), cols)
        out_ref[i] = jnp.transpose(zt[:, at].astype(F32) + result).astype(BF16)
        return carry

    lax.fori_loop(0, rows, attend, 0, unroll=4)

    for k in range(LAST):
        e_all(k).wait_send()


def fused(n, pair_rep, residue_mask, crop_length, norm_gain, mult_proj, mixed_gain, mult_out,
          att_gain, att_proj, att_bias, att_out):
    rows, cols, chans = pair_rep.shape
    heads = att_bias.shape[1]
    peers = n // 2
    mine = chans // n
    wide = chans // peers
    vm = pl.BlockSpec(memory_space=pltpu.VMEM)
    hbm = pl.BlockSpec(memory_space=pltpu.HBM)
    phases = FIRST + 2 * MIDDLE + SHARED + 3 * LAST
    few = mine // 2
    first = pltpu.VMEM((FIRST, 2 * peers, rows // FIRST * wide, cols), BF16)
    first_in = pltpu.VMEM((FIRST, 2 * n, rows // FIRST * wide, cols), BF16)
    back = pltpu.VMEM((MIDDLE, peers, rows // MIDDLE * wide, cols), BF16)
    second = pltpu.VMEM((MIDDLE, peers, 2, rows // MIDDLE * mine, cols), BF16)
    rest = pltpu.VMEM((SHARED, n, 2, rows // SHARED * few, cols), BF16)
    home = pltpu.VMEM((LAST, n, rows // LAST * mine, cols), BF16)
    home_few = pltpu.VMEM((LAST, n, rows // LAST * few, cols), BF16)
    bias = pltpu.VMEM((LAST, heads * rows // LAST, cols), BF16)
    bias_in = pltpu.VMEM((LAST, n, heads * rows // LAST, cols), BF16)

    def far(operand):
        return pltpu.with_memory_space_constraint(operand, pltpu.HBM)

    return pl.pallas_call(
        functools.partial(fused_kernel, n),
        out_shape=jax.ShapeDtypeStruct(pair_rep.shape, BF16),
        in_specs=[hbm, hbm, pl.BlockSpec(memory_space=pltpu.SMEM)] + [hbm] * 8,
        out_specs=vm,
        scratch_shapes=[
            pltpu.VMEM(pair_rep.shape, BF16),
            pltpu.VMEM((1, cols), jnp.int32),
            pltpu.VMEM(norm_gain.shape, F32),
            pltpu.VMEM(mult_proj.shape, BF16),
            pltpu.VMEM(mixed_gain.shape, F32),
            pltpu.VMEM(mult_out.shape, BF16),
            pltpu.VMEM((1, chans), F32),
            pltpu.VMEM(att_proj.shape, BF16),
            pltpu.VMEM((heads, chans), BF16),
            pltpu.VMEM(att_out.shape, BF16),
            pltpu.SemaphoreType.DMA((11,)),
            pltpu.VMEM((chans, rows * cols), BF16),
            pltpu.VMEM((chans, rows * cols), F32),
            pltpu.VMEM((n * rows * mine, cols), F32),
            pltpu.VMEM((n * rows * wide, cols), F32),
            pltpu.VMEM((n * rows * mine, cols), F32),
            pltpu.VMEM((2 * GROUP, chans), F32),
            pltpu.VMEM((cols, heads * cols), F32),
            pltpu.VMEM((rows, cols, chans), BF16),
            pltpu.VMEM((rows, chans, heads * cols), BF16),
            pltpu.VMEM((rows, chans, cols), BF16),
            pltpu.VMEM((rows, chans, cols), F32),
            pltpu.VMEM((rows, cols, heads * cols), F32),
            pltpu.VMEM((2, mult_proj.shape[2], chans), BF16),
            pltpu.VMEM((3, chans, chans), BF16),
            pltpu.VMEM((5, chans, cols), F32),
            pltpu.VMEM((3 * chans, chans), BF16),
            first,
            first_in,
            back,
            back,
            second,
            second,
            rest,
            rest,
            home,
            home,
            home_few,
            home_few,
            bias,
            bias_in,
            pltpu.SemaphoreType.DMA((phases,)),
            pltpu.SemaphoreType.DMA((phases,)),
        ],
        compiler_params=pltpu.CompilerParams(
            collective_id=0, has_side_effects=True, vmem_limit_bytes=48 * 1024 * 1024
        ),
        name="fused_pair",
    )(
        far(pair_rep),
        far(residue_mask.reshape(1, -1)),
        crop_length,
        far(norm_gain),
        far(mult_proj),
        far(mixed_gain),
        far(mult_out),
        far(att_gain.reshape(1, -1)),
        far(att_proj),
        far(att_bias.T),
        far(att_out),
    )


def choose(mesh):
    n = mesh.shape["row"]

    def body(pair_rep, *rest):
        rows, cols, chans = pair_rep.shape
        fits = (
            mesh.shape["col"] == 1
            and n & (n - 1) == 0
            and n > 1
            and chans == n * GROUP
            and rows == GROUP
            and cols == n * rows
            and cols == chans
        )
        if fits:
            return fused(n, pair_rep, *rest)
        return local(pair_rep, *rest)

    return body


def solution(mesh):
    placed = (
        P(("groups", "row"), "col", None),
        P("groups"),
        P("groups"),
        P(),
        P(),
        P(),
        P(),
        P(),
        P(),
        P(),
        P(),
    )
    return jax.shard_map(
        choose(mesh),
        mesh=mesh,
        in_specs=placed,
        out_specs=P(("groups", "row"), "col", None),
        check_vma=False,
    )
```

```python
import functools

import jax
import jax.numpy as jnp
from jax import lax
from jax.experimental import pallas as pl
from jax.experimental.pallas import tpu as pltpu
from jax.sharding import PartitionSpec as P

HID = 128
HEADS = 4
HEAD_DIM = 32
ATT = 128


EPSILON = 1e-05


def normalize(values, gain_vec, along):
    average = jnp.mean(values, axis=along, keepdims=True)
    centered = values - average
    variance = jnp.mean(centered * centered, axis=along, keepdims=True)
    return centered * lax.rsqrt(variance + EPSILON) * gain_vec


def outgoing_product(left_half, right_half):
    return lax.dot_general(
        left_half,
        lax.all_gather(right_half, "row", axis=1, tiled=True),
        (((2,), (2,)), ((0,), (0,))),
        preferred_element_type=jnp.float32,
    )


def incoming_product(left_half, right_half):
    left_cols, right_cols = (
        lax.all_to_all(left_half, "row", split_axis=2, concat_axis=1, tiled=True),
        lax.all_to_all(right_half, "row", split_axis=2, concat_axis=1, tiled=True),
    )
    return lax.dot_general(
        left_cols,
        lax.all_gather(right_cols, "row", axis=2, tiled=True),
        (((1,), (1,)), ((0,), (0,))),
        preferred_element_type=jnp.float32,
    )


def triangle_update(pair_rep, gain_vec, proj_w, out_gain, out_w, pair_mask, incoming):
    normed = normalize(pair_rep.astype(jnp.float32), gain_vec, 2).astype(jnp.bfloat16)
    channels = jnp.einsum(
        "ijd,de->eij", normed, proj_w[:, : 4 * HID], preferred_element_type=jnp.float32
    )
    gate_lin = jnp.einsum(
        "ijd,de->ije", normed, proj_w[:, 4 * HID :], preferred_element_type=jnp.float32
    )
    masked = pair_mask[None, :, :]
    left_proj = (masked * jax.nn.sigmoid(channels[HID : 2 * HID]) * channels[:HID]).astype(
        jnp.bfloat16
    )
    right_proj = (
        masked * jax.nn.sigmoid(channels[3 * HID : 4 * HID]) * channels[2 * HID : 3 * HID]
    ).astype(jnp.bfloat16)
    left_half, right_half = (
        lax.all_to_all(left_proj, "col", split_axis=0, concat_axis=2, tiled=True),
        lax.all_to_all(right_proj, "col", split_axis=0, concat_axis=2, tiled=True),
    )
    if incoming:
        product = incoming_product(left_half, right_half)
    else:
        product = outgoing_product(left_half, right_half)
    mixed = product.astype(jnp.bfloat16)
    mixed_tile = lax.all_to_all(mixed, "col", split_axis=2, concat_axis=0, tiled=True)
    mixed_norm = normalize(mixed_tile.astype(jnp.float32), out_gain[:, None, None], 0).astype(
        jnp.bfloat16
    )
    update = jnp.einsum("cij,cd->ijd", mixed_norm, out_w, preferred_element_type=jnp.float32)
    return (pair_rep.astype(jnp.float32) + jax.nn.sigmoid(gate_lin) * update).astype(jnp.bfloat16)


def local(
    pair_rep,
    residue_mask,
    crop_length,
    norm_gain,
    mult_proj,
    mixed_gain,
    mult_out,
    att_gain,
    att_proj,
    att_bias,
    att_out,
):
    row_count = pair_rep.shape[0]
    col_count = pair_rep.shape[1]
    row_start = lax.axis_index("row") * row_count
    col_start = lax.axis_index("col") * col_count
    positions = jnp.arange(residue_mask.shape[0], dtype=jnp.int32)
    alive = (((residue_mask == 1) | (positions == 0)) & (positions < crop_length[0])).astype(
        jnp.float32
    )
    row_alive = lax.dynamic_slice_in_dim(alive, row_start, row_count, 0)
    col_alive = lax.dynamic_slice_in_dim(alive, col_start, col_count, 0)
    pair_mask = row_alive[:, None] * col_alive[None, :]
    first = triangle_update(
        pair_rep, norm_gain[0], mult_proj[0], mixed_gain[0], mult_out[0], pair_mask, False
    )
    second = triangle_update(
        first, norm_gain[1], mult_proj[1], mixed_gain[1], mult_out[1], pair_mask, True
    )
    normed = normalize(second.astype(jnp.float32), att_gain, 2).astype(jnp.bfloat16)
    projected = jnp.einsum("ijd,de->ije", normed, att_proj, preferred_element_type=jnp.float32)
    queries = projected[..., :ATT].astype(jnp.bfloat16)
    key_rows = projected[..., ATT : 2 * ATT].astype(jnp.bfloat16)
    value_rows = projected[..., 2 * ATT : 3 * ATT].astype(jnp.bfloat16)
    gates = projected[..., 3 * ATT :].astype(jnp.bfloat16)
    bias_tile = jnp.einsum(
        "ijd,dh->hij", normed, att_bias, preferred_element_type=jnp.float32
    ).astype(jnp.bfloat16)
    key_all, value_all, bias_cols = (
        lax.all_gather(key_rows, "col", axis=1, tiled=True),
        lax.all_gather(value_rows, "col", axis=1, tiled=True),
        lax.all_gather(bias_tile, "col", axis=2, tiled=True),
    )
    bias_full = lax.all_gather(bias_cols, "row", axis=1, tiled=True)
    bias_mine = lax.dynamic_slice_in_dim(bias_full, col_start, col_count, 1).astype(jnp.float32)
    total = key_all.shape[1]
    key_mask = jnp.where(alive > 0, 0.0, -1000000000.0).astype(jnp.float32)
    scaling = 1.0 / float(HEAD_DIM) ** 0.5
    query_heads = queries.reshape(row_count, col_count, HEADS, HEAD_DIM)
    key_heads = key_all.reshape(row_count, total, HEADS, HEAD_DIM)
    value_heads = value_all.reshape(row_count, total, HEADS, HEAD_DIM)
    scores = jnp.einsum(
        "ijhd,ikhd->hijk", query_heads, key_heads, preferred_element_type=jnp.float32
    )
    scores = scores * scaling + bias_mine[:, None, :, :] + key_mask[None, None, None, :]
    weights = jax.nn.softmax(scores, axis=-1).astype(jnp.bfloat16)
    attended = jnp.einsum(
        "hijk,ikhd->ijhd", weights, value_heads, preferred_element_type=jnp.float32
    )
    attended = attended.reshape(row_count, col_count, ATT)
    gated = (jax.nn.sigmoid(gates.astype(jnp.float32)) * attended).astype(jnp.bfloat16)
    result = jnp.einsum("ija,ad->ijd", gated, att_out, preferred_element_type=jnp.float32)
    return (second.astype(jnp.float32) + result).astype(jnp.bfloat16)


MESH = pl.DeviceIdType.MESH
BF16 = jnp.bfloat16
F32 = jnp.float32
GROUP = 8
FIRST = 1
MIDDLE = 4
SHARED = 2
LAST = 2
MIXED = (15, 7, 11, 3, 14, 6, 10, 2, 13, 5, 9, 1, 12, 4, 8)
PAIRED = (15, 3, 14, 2, 13, 1, 12, 7, 11, 6, 10, 5, 9, 4, 8)
LOG2E = 1.4426950408889634


def sigmoid(x):
    return 0.5 * jnp.tanh(0.5 * x) + 0.5


def normalize_t(values, gain_col):
    average = jnp.mean(values, axis=0, keepdims=True)
    centered = values - average
    variance = jnp.mean(centered * centered, axis=0, keepdims=True)
    return centered * lax.rsqrt(variance + EPSILON) * gain_col


def mm(a, b, dims=((1,), (0,))):
    return lax.dot_general(a, b, (dims, ((), ())), preferred_element_type=F32)


def fused_kernel(
    n,
    pair_hbm,
    mask_hbm,
    crop_ref,
    gain_hbm,
    proj_hbm,
    mgain_hbm,
    mout_hbm,
    again_hbm,
    aproj_hbm,
    abias_hbm,
    aout_hbm,
    out_ref,
    pair_ref,
    mask_ref,
    gain_ref,
    proj_ref,
    mgain_ref,
    mout_ref,
    again_ref,
    aproj_ref,
    abias_ref,
    aout_ref,
    load_sem,
    zt,
    og,
    fx_left,
    fx_right,
    f_prod,
    b_pad,
    b_full,
    kmat,
    q_heads,
    vmat,
    gmat,
    scores,
    proj_t,
    out_t,
    gain_cols,
    qvg_t,
    send_a,
    recv_a,
    send_b,
    recv_b,
    send_c,
    recv_c,
    send_f,
    recv_f,
    send_d,
    recv_d,
    send_g,
    recv_g,
    send_e,
    recv_e,
    send_sem,
    recv_sem,
):
    me = lax.axis_index("row")
    rows, cols, chans = pair_ref.shape
    peers = n // 2
    mine = chans // n
    wide = chans // peers
    heads = abias_ref.shape[0]
    att = chans
    hid = chans
    dim = att // heads
    here = lax.rem(me, peers)
    near = me - here
    far = peers - near

    c_phase = FIRST + MIDDLE
    f_phase = c_phase + MIDDLE
    d_phase = f_phase + SHARED
    g_phase = d_phase + LAST
    e_phase = g_phase + LAST
    few = mine // 2

    barrier = pltpu.get_barrier_semaphore()
    for s in range(1, n):
        pl.semaphore_signal(
            barrier, inc=1, device_id={"row": lax.rem(me + s, n)}, device_id_type=MESH
        )

    loads = [
        pltpu.make_async_copy(src, dst, load_sem.at[at])
        for at, (src, dst) in enumerate((
            (mask_hbm, mask_ref),
            (gain_hbm, gain_ref),
            (proj_hbm.at[0], proj_ref.at[0]),
            (pair_hbm, pair_ref),
            (mgain_hbm, mgain_ref),
            (proj_hbm.at[1], proj_ref.at[1]),
            (mout_hbm, mout_ref),
            (again_hbm, again_ref),
            (aproj_hbm, aproj_ref),
            (abias_hbm, abias_ref),
            (aout_hbm, aout_ref),
        ))
    ]
    for load in loads:
        load.start()
    for load in loads[:4]:
        load.wait()

    def column(row_vec):
        return jnp.transpose(jnp.broadcast_to(row_vec.astype(F32), (chans, row_vec.shape[-1])))

    def flip(mat):
        return jnp.transpose(mat.astype(F32)).astype(BF16)

    lane = lax.broadcasted_iota(jnp.int32, (1, cols), 1)
    alive = jnp.where(
        ((mask_ref[...] == 1) | (lane == 0)) & (lane < crop_ref[0]), 1.0, 0.0
    ).astype(F32)

    def row_mask(i):
        own = jnp.where(lane == me * rows + i, alive, 0.0)
        return jnp.sum(own, axis=1, keepdims=True) * alive

    masks = [row_mask(i) for i in range(rows)]

    def at_row(i):
        return slice(i * cols, (i + 1) * cols)

    def chunk(k, parts):
        return range(k * rows // parts, (k + 1) * rows // parts)

    def remote(phase, src, dst, p):
        return pltpu.make_async_remote_copy(
            src_ref=src,
            dst_ref=dst,
            send_sem=send_sem.at[phase],
            recv_sem=recv_sem.at[phase],
            device_id={"row": p},
            device_id_type=MESH,
        )

    def partner(s):
        place, at = 1, 0
        while place < n:
            bit = lax.rem(lax.div(me, place) + s // place % 2, 2)
            at, place = at + place * bit, 2 * place
        return at

    def order(listed):
        return listed if len(listed) == n - 1 else range(n - 1, 0, -1)

    def a_both(k, p):
        src = send_a.at[k, pl.ds(2 * lax.rem(p, peers), 2)]
        return remote(k, src, recv_a.at[k, pl.ds(2 * me, 2)], p)

    def a_right(k, p):
        return remote(k, send_a.at[k, 2 * lax.rem(p, peers) + 1], recv_a.at[k, 2 * me + 1], p)

    def a_all(k):
        block = recv_a.at[k, : 2 * (peers - 1) + peers]
        return remote(k, block, block, me)

    def b_copy(k, p):
        return remote(FIRST + k, send_b.at[k, lax.rem(p, peers)], recv_b.at[k, here], p)

    def b_all(k):
        return remote(FIRST + k, send_b.at[k, : peers - 1], recv_b.at[k, : peers - 1], me)

    def c_copy(k, p):
        return remote(c_phase + k, send_c.at[k, lax.rem(p, peers)], recv_c.at[k, here], p)

    def c_all(k):
        return remote(c_phase + k, send_c.at[k, : peers - 1], recv_c.at[k, : peers - 1], me)

    def f_copy(k, p):
        return remote(f_phase + k, send_f.at[k, p], recv_f.at[k, me], p)

    def f_all(k):
        return remote(f_phase + k, send_f.at[k, : n - 1], recv_f.at[k, : n - 1], me)

    def d_copy(k, p):
        return remote(d_phase + k, send_d.at[k, p], recv_d.at[k, me], p)

    def d_all(k):
        return remote(d_phase + k, send_d.at[k, : n - 1], recv_d.at[k, : n - 1], me)

    def g_copy(k, p):
        return remote(g_phase + k, send_g.at[k, p], recv_g.at[k, me], p)

    def g_all(k):
        return remote(g_phase + k, send_g.at[k, : n - 1], recv_g.at[k, : n - 1], me)

    def e_copy(k, p):
        return remote(e_phase + k, send_e.at[k], recv_e.at[k, me], p)

    def e_all(k):
        block = recv_e.at[k, : n - 1]
        return remote(e_phase + k, block, block, me)

    def project(u, i):
        normed = normalize_t(zt[:, at_row(i)].astype(F32), gain_cols[u]).astype(BF16)
        pr = mm(proj_t[u], normed)
        left = masks[i] * sigmoid(pr[hid : 2 * hid]) * pr[:hid]
        right = masks[i] * sigmoid(pr[3 * hid : 4 * hid]) * pr[2 * hid : 3 * hid]
        og[:, at_row(i)] = sigmoid(pr[4 * hid :])
        return left, right

    def start_first(k):
        for r, i in enumerate(chunk(k, FIRST)):
            for side, half in enumerate(project(0, i)):
                parts = half.astype(BF16)
                for p in range(peers):
                    send_a[k, 2 * p + side, r * wide : (r + 1) * wide] = parts[
                        p * wide : (p + 1) * wide
                    ]
        if k == 0:
            pl.semaphore_wait(barrier, n - 1)
        for s in order(MIXED):
            (a_both if s < peers else a_right)(k, partner(s)).start()
        recv_a[k, pl.ds(2 * me, 2)] = send_a[k, pl.ds(2 * here, 2)]

    def multiply_first():
        span = rows // FIRST * wide
        for k in range(FIRST):
            a_all(k).wait_recv()
            for q in range(peers):
                at = q * rows * wide + k * span
                fx_left[at : at + span] = recv_a[k, 2 * (near + q)].astype(F32)
            for q in range(n):
                at = q * rows * wide + k * span
                fx_right[at : at + span] = recv_a[k, 2 * q + 1].astype(F32)
        for c in range(wide):
            at = pl.ds(c, peers * rows, stride=wide)
            a = fx_left[at, :].astype(BF16)
            b = fx_right[pl.ds(c, n * rows, stride=wide), :].astype(BF16)
            f_prod[at, :] = mm(a, b, ((1,), (1,)))
        span = rows // MIDDLE * wide
        for k in range(MIDDLE):
            for p in range(peers):
                send_b[k, p] = f_prod[pl.ds(p * rows * wide + k * span, span), :].astype(BF16)
            for s in range(peers - 1, 0, -1):
                b_copy(k, partner(s)).start()
            recv_b[k, here] = send_b[k, here]

    def finish(u, i, mixed):
        at = at_row(i)
        mixed_norm = normalize_t(mixed, gain_cols[2 + u]).astype(BF16)
        zt[:, at] = (zt[:, at].astype(F32) + og[:, at] * mm(out_t[u], mixed_norm)).astype(BF16)

    low = lax.broadcasted_iota(jnp.int32, (peers * mine, cols), 0) % mine < few

    def trade(x, y):
        x, y = x.reshape(peers * mine, cols), y.reshape(peers * mine, cols)
        up = pltpu.roll(x, peers * mine - few, 0)
        down = pltpu.roll(y, few, 0)
        pair = jnp.where(low, x, down), jnp.where(low, up, y)
        return [half.reshape(peers, mine, cols) for half in pair]

    shared = (([], []), ([], []))

    def turn(k):
        b_all(k).wait_recv()
        halves = ([], [])
        for r, i in enumerate(chunk(k, MIDDLE)):
            mixed = recv_b[k, :, r * wide : (r + 1) * wide].reshape(chans, cols).astype(F32)
            finish(0, i, mixed)
            for side, half in enumerate(project(1, i)):
                halves[side].append(half.reshape(peers, 2, mine, cols))
        for side in range(2):
            block = jnp.concatenate([half[:, 0] for half in halves[side]], axis=1)
            send_c[k, :, side] = block.astype(BF16)
            for r in range(0, rows // MIDDLE, 2):
                upper, lower = halves[side][r][:, 1], halves[side][r + 1][:, 1]
                for to, pair in enumerate(trade(upper, lower)):
                    shared[side][to].append(pair)
        for s in range(peers - 1, 0, -1):
            c_copy(k, partner(s)).start()
        recv_c[k, here] = send_c[k, here]
        if (k + 1) % (MIDDLE // SHARED) == 0:
            at = k * SHARED // MIDDLE
            for side in range(2):
                for to in range(2):
                    block = jnp.concatenate(shared[side][to], axis=1)
                    send_f[at, to * peers : (to + 1) * peers, side] = block.astype(BF16)
                    shared[side][to].clear()
            recv_f[at, me] = send_f[at, me]

    def partial_products():
        span = rows // MIDDLE * mine
        for k in range(MIDDLE):
            c_all(k).wait_recv()
            for q in range(peers):
                at = q * rows * mine + k * span
                fx_left[at : at + span] = recv_c[k, q, 0].astype(F32)
                fx_right[at : at + span] = recv_c[k, q, 1].astype(F32)
        for c in range(mine):
            at = pl.ds(c, peers * rows, stride=mine)
            a = fx_left[at, :].astype(BF16)
            b = fx_right[at, :].astype(BF16)
            f_prod[pl.ds(c, n * rows, stride=mine), :] = mm(a, b, ((0,), (0,)))
        span = rows // LAST * mine
        for k in range(LAST):
            for p in range(n):
                send_d[k, p] = f_prod[pl.ds(p * rows * mine + k * span, span), :].astype(BF16)
            recv_d[k, me] = send_d[k, me]
            if k == 0:
                for s in range(n - 1, 0, -1):
                    d_copy(k, partner(s)).start()

    def shared_products():
        span = rows // SHARED * few
        for k in range(SHARED):
            f_all(k).wait_recv()
            for q in range(n):
                at = q * rows * few + k * span
                fx_left[at : at + span] = recv_f[k, q, 0].astype(F32)
                fx_right[at : at + span] = recv_f[k, q, 1].astype(F32)
        for c in range(few):
            at = pl.ds(c, n * rows, stride=few)
            a = fx_left[at, :].astype(BF16)
            b = fx_right[at, :].astype(BF16)
            f_prod[at, :] = mm(a, b, ((0,), (0,)))
        span = rows // LAST * few
        for k in range(LAST):
            for p in range(n):
                send_g[k, p] = f_prod[pl.ds(p * rows * few + k * span, span), :].astype(BF16)
            if k > 0:
                for s in range(n - 1, 0, -1):
                    d_copy(k, partner(s)).start()
            for s in range(n - 1, 0, -1):
                g_copy(k, partner(s)).start()
            recv_g[k, me] = send_g[k, me]

    def close(k):
        d_all(k).wait_recv()
        both = recv_d[k].astype(F32)
        summed = both[:peers] + both[peers:]
        g_all(k).wait_recv()
        ends = recv_g[k].astype(F32)
        tails = []
        for r in range(0, rows // LAST, 2):
            pair = ends[:, r * few : (r + 2) * few]
            tails += trade(pair[:peers], pair[peers:])
        biases = []
        normed_rows = []
        for r, i in enumerate(chunk(k, LAST)):
            mixed = jnp.concatenate([summed[:, r * mine : (r + 1) * mine], tails[r]], axis=1)
            finish(1, i, mixed.reshape(chans, cols))
            normed = normalize_t(zt[:, at_row(i)].astype(F32), gain_cols[4]).astype(BF16)
            normed_rows.append(normed)
            biases.append(mm(b_pad[...].astype(BF16), normed))
        send_e[k] = jnp.concatenate(
            [row[h : h + 1] for h in range(heads) for row in biases], axis=0
        ).astype(BF16)
        for s in range(n - 1, 0, -1):
            e_copy(k, partner(s)).start()
        recv_e[k, me] = send_e[k]
        return normed_rows

    def attention_inputs(k, normed_rows):
        for i, normed in zip(chunk(k, LAST), normed_rows):
            kmat[i] = mm(flip(normed), aproj_ref[:, att : 2 * att]).astype(BF16)
            qvg = mm(qvg_t[...], normed).astype(BF16)
            for h in range(heads):
                ch = slice(h * dim, (h + 1) * dim)
                q_heads[i, ch, h * cols : (h + 1) * cols] = qvg[ch]
            vmat[i] = qvg[att : 2 * att]
            gmat[i] = sigmoid(qvg[2 * att :].astype(F32))
            scores[i] = mm(kmat[i], q_heads[i]) * (LOG2E / float(dim) ** 0.5)

    gain_cols[0] = column(gain_ref[0:1, :])
    proj_t[0] = flip(proj_ref[0])
    for i in range(rows):
        zt[:, at_row(i)] = flip(pair_ref[i])
    for k in range(FIRST):
        start_first(k)
    for load in loads[4:]:
        load.wait()
    gain_cols[1] = column(gain_ref[1:2, :])
    gain_cols[2] = column(mgain_ref[0:1, :])
    gain_cols[3] = column(mgain_ref[1:2, :])
    gain_cols[4] = column(again_ref[...])
    proj_t[1] = flip(proj_ref[1])
    for u in range(2):
        out_t[u] = flip(mout_ref[u])
    out_t[2] = flip(aout_ref[...])
    qvg_t[:att] = flip(aproj_ref[:, :att])
    qvg_t[att:] = flip(aproj_ref[:, 2 * att :])
    b_pad[...] = jnp.zeros_like(b_pad)
    b_pad[:heads] = abias_ref[...].astype(F32)
    q_heads[...] = jnp.zeros_like(q_heads)
    key_mask = column(jnp.where(alive > 0, 0.0, -1000000000.0))
    multiply_first()
    for k in range(MIDDLE):
        turn(k)
    for k in range(SHARED):
        for s in order(PAIRED):
            f_copy(k, partner(s)).start()
    for k in range(FIRST):
        a_all(k).wait_send()
    for k in range(MIDDLE):
        b_all(k).wait_send()
    partial_products()
    shared_products()
    for k in range(MIDDLE):
        c_all(k).wait_send()
    for k in range(SHARED):
        f_all(k).wait_send()
    for k in range(LAST):
        attention_inputs(k, close(k))
    for k in range(LAST):
        d_all(k).wait_send()
        g_all(k).wait_send()

    for k in range(LAST):
        e_all(k).wait_recv()
    part = rows // LAST
    for h in range(heads):
        pieces = []
        for q in range(n):
            for k in range(LAST):
                pieces.append(recv_e[k, q].astype(F32)[h * part : (h + 1) * part])
        across = jnp.transpose(jnp.concatenate(pieces, axis=0))
        b_full[:, h * cols : (h + 1) * cols] = (across + key_mask) * LOG2E

    def attend(i, carry):
        parts = []
        for h in range(heads):
            at = slice(h * cols, (h + 1) * cols)
            total = scores[i, :, at] + b_full[:, at]
            e = jnp.exp2(total - jnp.max(total, axis=0, keepdims=True))
            inverse = 1.0 / jnp.sum(e, axis=0, keepdims=True)
            parts.append(mm(vmat[i, h * dim : (h + 1) * dim, :], e.astype(BF16)) * inverse)
        attended = jnp.concatenate(parts, axis=0)
        gated = (gmat[i] * attended).astype(BF16)
        result = mm(out_t[2], gated)
        at = pl.ds(pl.multiple_of(i * cols, cols), cols)
        out_ref[i] = jnp.transpose(zt[:, at].astype(F32) + result).astype(BF16)
        return carry

    lax.fori_loop(0, rows, attend, 0, unroll=8)

    for k in range(LAST):
        e_all(k).wait_send()


def fused(n, pair_rep, residue_mask, crop_length, norm_gain, mult_proj, mixed_gain, mult_out,
          att_gain, att_proj, att_bias, att_out):
    rows, cols, chans = pair_rep.shape
    heads = att_bias.shape[1]
    peers = n // 2
    mine = chans // n
    wide = chans // peers
    vm = pl.BlockSpec(memory_space=pltpu.VMEM)
    hbm = pl.BlockSpec(memory_space=pltpu.HBM)
    phases = FIRST + 2 * MIDDLE + SHARED + 3 * LAST
    few = mine // 2
    first = pltpu.VMEM((FIRST, 2 * peers, rows // FIRST * wide, cols), BF16)
    first_in = pltpu.VMEM((FIRST, 2 * n, rows // FIRST * wide, cols), BF16)
    back = pltpu.VMEM((MIDDLE, peers, rows // MIDDLE * wide, cols), BF16)
    second = pltpu.VMEM((MIDDLE, peers, 2, rows // MIDDLE * mine, cols), BF16)
    rest = pltpu.VMEM((SHARED, n, 2, rows // SHARED * few, cols), BF16)
    home = pltpu.VMEM((LAST, n, rows // LAST * mine, cols), BF16)
    home_few = pltpu.VMEM((LAST, n, rows // LAST * few, cols), BF16)
    bias = pltpu.VMEM((LAST, heads * rows // LAST, cols), BF16)
    bias_in = pltpu.VMEM((LAST, n, heads * rows // LAST, cols), BF16)

    def far(operand):
        return pltpu.with_memory_space_constraint(operand, pltpu.HBM)

    return pl.pallas_call(
        functools.partial(fused_kernel, n),
        out_shape=jax.ShapeDtypeStruct(pair_rep.shape, BF16),
        in_specs=[hbm, hbm, pl.BlockSpec(memory_space=pltpu.SMEM)] + [hbm] * 8,
        out_specs=vm,
        scratch_shapes=[
            pltpu.VMEM(pair_rep.shape, BF16),
            pltpu.VMEM((1, cols), jnp.int32),
            pltpu.VMEM(norm_gain.shape, F32),
            pltpu.VMEM(mult_proj.shape, BF16),
            pltpu.VMEM(mixed_gain.shape, F32),
            pltpu.VMEM(mult_out.shape, BF16),
            pltpu.VMEM((1, chans), F32),
            pltpu.VMEM(att_proj.shape, BF16),
            pltpu.VMEM((heads, chans), BF16),
            pltpu.VMEM(att_out.shape, BF16),
            pltpu.SemaphoreType.DMA((11,)),
            pltpu.VMEM((chans, rows * cols), BF16),
            pltpu.VMEM((chans, rows * cols), F32),
            pltpu.VMEM((n * rows * mine, cols), F32),
            pltpu.VMEM((n * rows * wide, cols), F32),
            pltpu.VMEM((n * rows * mine, cols), F32),
            pltpu.VMEM((2 * GROUP, chans), F32),
            pltpu.VMEM((cols, heads * cols), F32),
            pltpu.VMEM((rows, cols, chans), BF16),
            pltpu.VMEM((rows, chans, heads * cols), BF16),
            pltpu.VMEM((rows, chans, cols), BF16),
            pltpu.VMEM((rows, chans, cols), F32),
            pltpu.VMEM((rows, cols, heads * cols), F32),
            pltpu.VMEM((2, mult_proj.shape[2], chans), BF16),
            pltpu.VMEM((3, chans, chans), BF16),
            pltpu.VMEM((5, chans, cols), F32),
            pltpu.VMEM((3 * chans, chans), BF16),
            first,
            first_in,
            back,
            back,
            second,
            second,
            rest,
            rest,
            home,
            home,
            home_few,
            home_few,
            bias,
            bias_in,
            pltpu.SemaphoreType.DMA((phases,)),
            pltpu.SemaphoreType.DMA((phases,)),
        ],
        compiler_params=pltpu.CompilerParams(
            collective_id=0, has_side_effects=True, vmem_limit_bytes=48 * 1024 * 1024
        ),
        name="fused_pair",
    )(
        far(pair_rep),
        far(residue_mask.reshape(1, -1)),
        crop_length,
        far(norm_gain),
        far(mult_proj),
        far(mixed_gain),
        far(mult_out),
        far(att_gain.reshape(1, -1)),
        far(att_proj),
        far(att_bias.T),
        far(att_out),
    )


def choose(mesh):
    n = mesh.shape["row"]

    def body(pair_rep, *rest):
        rows, cols, chans = pair_rep.shape
        fits = (
            mesh.shape["col"] == 1
            and n & (n - 1) == 0
            and n > 1
            and chans == n * GROUP
            and rows == GROUP
            and cols == n * rows
            and cols == chans
        )
        if fits:
            return fused(n, pair_rep, *rest)
        return local(pair_rep, *rest)

    return body


def solution(mesh):
    placed = (
        P(("groups", "row"), "col", None),
        P("groups"),
        P("groups"),
        P(),
        P(),
        P(),
        P(),
        P(),
        P(),
        P(),
        P(),
    )
    return jax.shard_map(
        choose(mesh),
        mesh=mesh,
        in_specs=placed,
        out_specs=P(("groups", "row"), "col", None),
        check_vma=False,
    )
```

```python
import functools

import jax
import jax.numpy as jnp
from jax import lax
from jax.experimental import pallas as pl
from jax.experimental.pallas import tpu as pltpu
from jax.sharding import PartitionSpec as P

HID = 128
HEADS = 4
HEAD_DIM = 32
ATT = 128


EPSILON = 1e-05


def normalize(values, gain_vec, along):
    average = jnp.mean(values, axis=along, keepdims=True)
    centered = values - average
    variance = jnp.mean(centered * centered, axis=along, keepdims=True)
    return centered * lax.rsqrt(variance + EPSILON) * gain_vec


def outgoing_product(left_half, right_half):
    return lax.dot_general(
        left_half,
        lax.all_gather(right_half, "row", axis=1, tiled=True),
        (((2,), (2,)), ((0,), (0,))),
        preferred_element_type=jnp.float32,
    )


def incoming_product(left_half, right_half):
    left_cols, right_cols = (
        lax.all_to_all(left_half, "row", split_axis=2, concat_axis=1, tiled=True),
        lax.all_to_all(right_half, "row", split_axis=2, concat_axis=1, tiled=True),
    )
    return lax.dot_general(
        left_cols,
        lax.all_gather(right_cols, "row", axis=2, tiled=True),
        (((1,), (1,)), ((0,), (0,))),
        preferred_element_type=jnp.float32,
    )


def triangle_update(pair_rep, gain_vec, proj_w, out_gain, out_w, pair_mask, incoming):
    normed = normalize(pair_rep.astype(jnp.float32), gain_vec, 2).astype(jnp.bfloat16)
    channels = jnp.einsum(
        "ijd,de->eij", normed, proj_w[:, : 4 * HID], preferred_element_type=jnp.float32
    )
    gate_lin = jnp.einsum(
        "ijd,de->ije", normed, proj_w[:, 4 * HID :], preferred_element_type=jnp.float32
    )
    masked = pair_mask[None, :, :]
    left_proj = (masked * jax.nn.sigmoid(channels[HID : 2 * HID]) * channels[:HID]).astype(
        jnp.bfloat16
    )
    right_proj = (
        masked * jax.nn.sigmoid(channels[3 * HID : 4 * HID]) * channels[2 * HID : 3 * HID]
    ).astype(jnp.bfloat16)
    left_half, right_half = (
        lax.all_to_all(left_proj, "col", split_axis=0, concat_axis=2, tiled=True),
        lax.all_to_all(right_proj, "col", split_axis=0, concat_axis=2, tiled=True),
    )
    if incoming:
        product = incoming_product(left_half, right_half)
    else:
        product = outgoing_product(left_half, right_half)
    mixed = product.astype(jnp.bfloat16)
    mixed_tile = lax.all_to_all(mixed, "col", split_axis=2, concat_axis=0, tiled=True)
    mixed_norm = normalize(mixed_tile.astype(jnp.float32), out_gain[:, None, None], 0).astype(
        jnp.bfloat16
    )
    update = jnp.einsum("cij,cd->ijd", mixed_norm, out_w, preferred_element_type=jnp.float32)
    return (pair_rep.astype(jnp.float32) + jax.nn.sigmoid(gate_lin) * update).astype(jnp.bfloat16)


def local(
    pair_rep,
    residue_mask,
    crop_length,
    norm_gain,
    mult_proj,
    mixed_gain,
    mult_out,
    att_gain,
    att_proj,
    att_bias,
    att_out,
):
    row_count = pair_rep.shape[0]
    col_count = pair_rep.shape[1]
    row_start = lax.axis_index("row") * row_count
    col_start = lax.axis_index("col") * col_count
    positions = jnp.arange(residue_mask.shape[0], dtype=jnp.int32)
    alive = (((residue_mask == 1) | (positions == 0)) & (positions < crop_length[0])).astype(
        jnp.float32
    )
    row_alive = lax.dynamic_slice_in_dim(alive, row_start, row_count, 0)
    col_alive = lax.dynamic_slice_in_dim(alive, col_start, col_count, 0)
    pair_mask = row_alive[:, None] * col_alive[None, :]
    first = triangle_update(
        pair_rep, norm_gain[0], mult_proj[0], mixed_gain[0], mult_out[0], pair_mask, False
    )
    second = triangle_update(
        first, norm_gain[1], mult_proj[1], mixed_gain[1], mult_out[1], pair_mask, True
    )
    normed = normalize(second.astype(jnp.float32), att_gain, 2).astype(jnp.bfloat16)
    projected = jnp.einsum("ijd,de->ije", normed, att_proj, preferred_element_type=jnp.float32)
    queries = projected[..., :ATT].astype(jnp.bfloat16)
    key_rows = projected[..., ATT : 2 * ATT].astype(jnp.bfloat16)
    value_rows = projected[..., 2 * ATT : 3 * ATT].astype(jnp.bfloat16)
    gates = projected[..., 3 * ATT :].astype(jnp.bfloat16)
    bias_tile = jnp.einsum(
        "ijd,dh->hij", normed, att_bias, preferred_element_type=jnp.float32
    ).astype(jnp.bfloat16)
    key_all, value_all, bias_cols = (
        lax.all_gather(key_rows, "col", axis=1, tiled=True),
        lax.all_gather(value_rows, "col", axis=1, tiled=True),
        lax.all_gather(bias_tile, "col", axis=2, tiled=True),
    )
    bias_full = lax.all_gather(bias_cols, "row", axis=1, tiled=True)
    bias_mine = lax.dynamic_slice_in_dim(bias_full, col_start, col_count, 1).astype(jnp.float32)
    total = key_all.shape[1]
    key_mask = jnp.where(alive > 0, 0.0, -1000000000.0).astype(jnp.float32)
    scaling = 1.0 / float(HEAD_DIM) ** 0.5
    query_heads = queries.reshape(row_count, col_count, HEADS, HEAD_DIM)
    key_heads = key_all.reshape(row_count, total, HEADS, HEAD_DIM)
    value_heads = value_all.reshape(row_count, total, HEADS, HEAD_DIM)
    scores = jnp.einsum(
        "ijhd,ikhd->hijk", query_heads, key_heads, preferred_element_type=jnp.float32
    )
    scores = scores * scaling + bias_mine[:, None, :, :] + key_mask[None, None, None, :]
    weights = jax.nn.softmax(scores, axis=-1).astype(jnp.bfloat16)
    attended = jnp.einsum(
        "hijk,ikhd->ijhd", weights, value_heads, preferred_element_type=jnp.float32
    )
    attended = attended.reshape(row_count, col_count, ATT)
    gated = (jax.nn.sigmoid(gates.astype(jnp.float32)) * attended).astype(jnp.bfloat16)
    result = jnp.einsum("ija,ad->ijd", gated, att_out, preferred_element_type=jnp.float32)
    return (second.astype(jnp.float32) + result).astype(jnp.bfloat16)


MESH = pl.DeviceIdType.MESH
BF16 = jnp.bfloat16
F32 = jnp.float32
GROUP = 8
FIRST = 1
MIDDLE = 4
SHARED = 2
LAST = 2
MIXED = (15, 7, 11, 3, 14, 6, 10, 2, 13, 5, 9, 1, 12, 4, 8)
PAIRED = (15, 3, 14, 2, 13, 1, 12, 7, 11, 6, 10, 5, 9, 4, 8)
LOG2E = 1.4426950408889634


def sigmoid(x):
    return 0.5 * jnp.tanh(0.5 * x) + 0.5


def normalize_t(values, gain_col):
    average = jnp.mean(values, axis=0, keepdims=True)
    centered = values - average
    variance = jnp.mean(centered * centered, axis=0, keepdims=True)
    return centered * lax.rsqrt(variance + EPSILON) * gain_col


def mm(a, b, dims=((1,), (0,))):
    return lax.dot_general(a, b, (dims, ((), ())), preferred_element_type=F32)


def fused_kernel(
    n,
    pair_hbm,
    mask_hbm,
    crop_ref,
    gain_hbm,
    proj_hbm,
    mgain_hbm,
    mout_hbm,
    again_hbm,
    aproj_hbm,
    abias_hbm,
    aout_hbm,
    out_ref,
    pair_ref,
    mask_ref,
    gain_ref,
    proj_ref,
    mgain_ref,
    mout_ref,
    again_ref,
    aproj_ref,
    abias_ref,
    aout_ref,
    load_sem,
    zt,
    og,
    fx_left,
    fx_right,
    f_prod,
    b_pad,
    b_full,
    kmat,
    q_heads,
    vmat,
    gmat,
    scores,
    proj_t,
    out_t,
    gain_cols,
    qvg_t,
    send_a,
    recv_a,
    send_b,
    recv_b,
    send_c,
    recv_c,
    send_f,
    recv_f,
    send_d,
    recv_d,
    send_g,
    recv_g,
    send_e,
    recv_e,
    send_sem,
    recv_sem,
):
    me = lax.axis_index("row")
    rows, cols, chans = pair_ref.shape
    peers = n // 2
    mine = chans // n
    wide = chans // peers
    heads = abias_ref.shape[0]
    att = chans
    hid = chans
    dim = att // heads
    here = lax.rem(me, peers)
    near = me - here
    far = peers - near

    c_phase = FIRST + MIDDLE
    f_phase = c_phase + MIDDLE
    d_phase = f_phase + SHARED
    g_phase = d_phase + LAST
    e_phase = g_phase + LAST
    a_phase = e_phase + LAST
    few = mine // 2

    barrier = pltpu.get_barrier_semaphore()
    for s in range(1, n):
        pl.semaphore_signal(
            barrier, inc=1, device_id={"row": lax.rem(me + s, n)}, device_id_type=MESH
        )

    loads = [
        pltpu.make_async_copy(src, dst, load_sem.at[at])
        for at, (src, dst) in enumerate((
            (mask_hbm, mask_ref),
            (gain_hbm, gain_ref),
            (proj_hbm.at[0], proj_ref.at[0]),
            (pair_hbm, pair_ref),
            (mgain_hbm, mgain_ref),
            (proj_hbm.at[1], proj_ref.at[1]),
            (mout_hbm, mout_ref),
            (again_hbm, again_ref),
            (aproj_hbm, aproj_ref),
            (abias_hbm, abias_ref),
            (aout_hbm, aout_ref),
        ))
    ]
    for load in loads:
        load.start()
    for load in loads[:4]:
        load.wait()

    def column(row_vec):
        return jnp.transpose(jnp.broadcast_to(row_vec.astype(F32), (chans, row_vec.shape[-1])))

    def flip(mat):
        return jnp.transpose(mat.astype(F32)).astype(BF16)

    lane = lax.broadcasted_iota(jnp.int32, (1, cols), 1)
    alive = jnp.where(
        ((mask_ref[...] == 1) | (lane == 0)) & (lane < crop_ref[0]), 1.0, 0.0
    ).astype(F32)

    def row_mask(i):
        own = jnp.where(lane == me * rows + i, alive, 0.0)
        return jnp.sum(own, axis=1, keepdims=True) * alive

    masks = [row_mask(i) for i in range(rows)]

    def at_row(i):
        return slice(i * cols, (i + 1) * cols)

    def chunk(k, parts):
        return range(k * rows // parts, (k + 1) * rows // parts)

    def remote(phase, src, dst, p):
        return pltpu.make_async_remote_copy(
            src_ref=src,
            dst_ref=dst,
            send_sem=send_sem.at[phase],
            recv_sem=recv_sem.at[phase],
            device_id={"row": p},
            device_id_type=MESH,
        )

    def partner(s):
        place, at = 1, 0
        while place < n:
            bit = lax.rem(lax.div(me, place) + s // place % 2, 2)
            at, place = at + place * bit, 2 * place
        return at

    def order(listed):
        return listed if len(listed) == n - 1 else range(n - 1, 0, -1)

    def a_both(k, p):
        src = send_a.at[k, pl.ds(2 * lax.rem(p, peers), 2)]
        return remote(k, src, recv_a.at[k, pl.ds(2 * me, 2)], p)

    def a_right(k, p):
        return remote(
            a_phase + k, send_a.at[k, 2 * lax.rem(p, peers) + 1], recv_a.at[k, 2 * me + 1], p
        )

    def a_near(k):
        block = recv_a.at[k, : 2 * (peers - 1)]
        return remote(k, block, block, me)

    def a_far(k):
        block = recv_a.at[k, :peers]
        return remote(a_phase + k, block, block, me)

    def b_copy(k, p):
        return remote(FIRST + k, send_b.at[k, lax.rem(p, peers)], recv_b.at[k, here], p)

    def b_all(k):
        return remote(FIRST + k, send_b.at[k, : peers - 1], recv_b.at[k, : peers - 1], me)

    def c_copy(k, p):
        return remote(c_phase + k, send_c.at[k, lax.rem(p, peers)], recv_c.at[k, here], p)

    def c_all(k):
        return remote(c_phase + k, send_c.at[k, : peers - 1], recv_c.at[k, : peers - 1], me)

    def f_copy(k, p):
        return remote(f_phase + k, send_f.at[k, p], recv_f.at[k, me], p)

    def f_all(k):
        return remote(f_phase + k, send_f.at[k, : n - 1], recv_f.at[k, : n - 1], me)

    def d_copy(k, p):
        return remote(d_phase + k, send_d.at[k, p], recv_d.at[k, me], p)

    def d_all(k):
        return remote(d_phase + k, send_d.at[k, : n - 1], recv_d.at[k, : n - 1], me)

    def g_copy(k, p):
        return remote(g_phase + k, send_g.at[k, p], recv_g.at[k, me], p)

    def g_all(k):
        return remote(g_phase + k, send_g.at[k, : n - 1], recv_g.at[k, : n - 1], me)

    def e_copy(k, p):
        return remote(e_phase + k, send_e.at[k], recv_e.at[k, me], p)

    def e_all(k):
        block = recv_e.at[k, : n - 1]
        return remote(e_phase + k, block, block, me)

    def project(u, i):
        normed = normalize_t(zt[:, at_row(i)].astype(F32), gain_cols[u]).astype(BF16)
        pr = mm(proj_t[u, : 4 * hid], normed)
        left = masks[i] * sigmoid(pr[hid : 2 * hid]) * pr[:hid]
        right = masks[i] * sigmoid(pr[3 * hid : 4 * hid]) * pr[2 * hid : 3 * hid]
        return left, right

    def gates(u):
        for i in range(rows):
            normed = normalize_t(zt[:, at_row(i)].astype(F32), gain_cols[u]).astype(BF16)
            og[:, at_row(i)] = sigmoid(mm(proj_t[u, 4 * hid :], normed))

    def start_first(k):
        for r, i in enumerate(chunk(k, FIRST)):
            for side, half in enumerate(project(0, i)):
                parts = half.astype(BF16)
                for p in range(peers):
                    send_a[k, 2 * p + side, r * wide : (r + 1) * wide] = parts[
                        p * wide : (p + 1) * wide
                    ]
        if k == 0:
            pl.semaphore_wait(barrier, n - 1)
        for s in order(MIXED):
            (a_both if s < peers else a_right)(k, partner(s)).start()
        recv_a[k, pl.ds(2 * me, 2)] = send_a[k, pl.ds(2 * here, 2)]

    def multiply_first():
        span = rows // FIRST * wide
        for k in range(FIRST):
            a_far(k).wait_recv()
            for q in range(peers):
                at = pl.multiple_of((far + q) * rows * wide + k * span, span)
                fx_right[pl.ds(at, span)] = recv_a[k, 2 * (far + q) + 1].astype(F32)
            a_near(k).wait_recv()
            for q in range(peers):
                at = q * rows * wide + k * span
                fx_left[at : at + span] = recv_a[k, 2 * (near + q)].astype(F32)
                at = pl.multiple_of((near + q) * rows * wide + k * span, span)
                fx_right[pl.ds(at, span)] = recv_a[k, 2 * (near + q) + 1].astype(F32)
        for c in range(wide):
            at = pl.ds(c, peers * rows, stride=wide)
            a = fx_left[at, :].astype(BF16)
            b = fx_right[pl.ds(c, n * rows, stride=wide), :].astype(BF16)
            f_prod[at, :] = mm(a, b, ((1,), (1,)))
        span = rows // MIDDLE * wide
        for k in range(MIDDLE):
            for p in range(peers):
                send_b[k, p] = f_prod[pl.ds(p * rows * wide + k * span, span), :].astype(BF16)
            for s in range(peers - 1, 0, -1):
                b_copy(k, partner(s)).start()
            recv_b[k, here] = send_b[k, here]

    def finish(u, i, mixed):
        at = at_row(i)
        mixed_norm = normalize_t(mixed, gain_cols[2 + u]).astype(BF16)
        zt[:, at] = (zt[:, at].astype(F32) + og[:, at] * mm(out_t[u], mixed_norm)).astype(BF16)

    low = lax.broadcasted_iota(jnp.int32, (peers * mine, cols), 0) % mine < few

    def trade(x, y):
        x, y = x.reshape(peers * mine, cols), y.reshape(peers * mine, cols)
        up = pltpu.roll(x, peers * mine - few, 0)
        down = pltpu.roll(y, few, 0)
        pair = jnp.where(low, x, down), jnp.where(low, up, y)
        return [half.reshape(peers, mine, cols) for half in pair]

    shared = (([], []), ([], []))

    def turn(k):
        b_all(k).wait_recv()
        halves = ([], [])
        for r, i in enumerate(chunk(k, MIDDLE)):
            mixed = recv_b[k, :, r * wide : (r + 1) * wide].reshape(chans, cols).astype(F32)
            finish(0, i, mixed)
            for side, half in enumerate(project(1, i)):
                halves[side].append(half.reshape(peers, 2, mine, cols))
        for side in range(2):
            block = jnp.concatenate([half[:, 0] for half in halves[side]], axis=1)
            send_c[k, :, side] = block.astype(BF16)
            for r in range(0, rows // MIDDLE, 2):
                upper, lower = halves[side][r][:, 1], halves[side][r + 1][:, 1]
                for to, pair in enumerate(trade(upper, lower)):
                    shared[side][to].append(pair)
        for s in range(peers - 1, 0, -1):
            c_copy(k, partner(s)).start()
        recv_c[k, here] = send_c[k, here]
        if (k + 1) % (MIDDLE // SHARED) == 0:
            at = k * SHARED // MIDDLE
            for side in range(2):
                for to in range(2):
                    block = jnp.concatenate(shared[side][to], axis=1)
                    send_f[at, to * peers : (to + 1) * peers, side] = block.astype(BF16)
                    shared[side][to].clear()
            recv_f[at, me] = send_f[at, me]

    def partial_products():
        span = rows // MIDDLE * mine
        for k in range(MIDDLE):
            c_all(k).wait_recv()
            for q in range(peers):
                at = q * rows * mine + k * span
                fx_left[at : at + span] = recv_c[k, q, 0].astype(F32)
                fx_right[at : at + span] = recv_c[k, q, 1].astype(F32)
        for c in range(mine):
            at = pl.ds(c, peers * rows, stride=mine)
            a = fx_left[at, :].astype(BF16)
            b = fx_right[at, :].astype(BF16)
            f_prod[pl.ds(c, n * rows, stride=mine), :] = mm(a, b, ((0,), (0,)))
        span = rows // LAST * mine
        for k in range(LAST):
            for p in range(n):
                send_d[k, p] = f_prod[pl.ds(p * rows * mine + k * span, span), :].astype(BF16)
            recv_d[k, me] = send_d[k, me]
            if k == 0:
                for s in range(n - 1, 0, -1):
                    d_copy(k, partner(s)).start()

    def shared_products():
        span = rows // SHARED * few
        for k in range(SHARED):
            f_all(k).wait_recv()
            for q in range(n):
                at = q * rows * few + k * span
                fx_left[at : at + span] = recv_f[k, q, 0].astype(F32)
                fx_right[at : at + span] = recv_f[k, q, 1].astype(F32)
        for c in range(few):
            at = pl.ds(c, n * rows, stride=few)
            a = fx_left[at, :].astype(BF16)
            b = fx_right[at, :].astype(BF16)
            f_prod[at, :] = mm(a, b, ((0,), (0,)))
        span = rows // LAST * few
        for k in range(LAST):
            for p in range(n):
                send_g[k, p] = f_prod[pl.ds(p * rows * few + k * span, span), :].astype(BF16)
            if k > 0:
                for s in range(n - 1, 0, -1):
                    d_copy(k, partner(s)).start()
            for s in range(n - 1, 0, -1):
                g_copy(k, partner(s)).start()
            recv_g[k, me] = send_g[k, me]

    def close(k):
        d_all(k).wait_recv()
        both = recv_d[k].astype(F32)
        summed = both[:peers] + both[peers:]
        g_all(k).wait_recv()
        ends = recv_g[k].astype(F32)
        tails = []
        for r in range(0, rows // LAST, 2):
            pair = ends[:, r * few : (r + 2) * few]
            tails += trade(pair[:peers], pair[peers:])
        biases = []
        normed_rows = []
        for r, i in enumerate(chunk(k, LAST)):
            mixed = jnp.concatenate([summed[:, r * mine : (r + 1) * mine], tails[r]], axis=1)
            finish(1, i, mixed.reshape(chans, cols))
            normed = normalize_t(zt[:, at_row(i)].astype(F32), gain_cols[4]).astype(BF16)
            normed_rows.append(normed)
            biases.append(mm(b_pad[...].astype(BF16), normed))
        send_e[k] = jnp.concatenate(
            [row[h : h + 1] for h in range(heads) for row in biases], axis=0
        ).astype(BF16)
        for s in range(n - 1, 0, -1):
            e_copy(k, partner(s)).start()
        recv_e[k, me] = send_e[k]
        return normed_rows

    def attention_inputs(k, normed_rows):
        for i, normed in zip(chunk(k, LAST), normed_rows):
            kmat[i] = mm(flip(normed), aproj_ref[:, att : 2 * att]).astype(BF16)
            qvg = mm(qvg_t[...], normed).astype(BF16)
            for h in range(heads):
                ch = slice(h * dim, (h + 1) * dim)
                q_heads[i, ch, h * cols : (h + 1) * cols] = qvg[ch]
            vmat[i] = qvg[att : 2 * att]
            gmat[i] = sigmoid(qvg[2 * att :].astype(F32))
            scores[i] = mm(kmat[i], q_heads[i]) * (LOG2E / float(dim) ** 0.5)

    gain_cols[0] = column(gain_ref[0:1, :])
    proj_t[0, : 4 * hid] = flip(proj_ref[0, :, : 4 * hid])
    for i in range(rows):
        zt[:, at_row(i)] = flip(pair_ref[i])
    for k in range(FIRST):
        start_first(k)
    for load in loads[4:]:
        load.wait()
    proj_t[0, 4 * hid :] = flip(proj_ref[0, :, 4 * hid :])
    gates(0)
    gain_cols[1] = column(gain_ref[1:2, :])
    gain_cols[2] = column(mgain_ref[0:1, :])
    gain_cols[3] = column(mgain_ref[1:2, :])
    gain_cols[4] = column(again_ref[...])
    proj_t[1] = flip(proj_ref[1])
    for u in range(2):
        out_t[u] = flip(mout_ref[u])
    out_t[2] = flip(aout_ref[...])
    qvg_t[:att] = flip(aproj_ref[:, :att])
    qvg_t[att:] = flip(aproj_ref[:, 2 * att :])
    b_pad[...] = jnp.zeros_like(b_pad)
    b_pad[:heads] = abias_ref[...].astype(F32)
    q_heads[...] = jnp.zeros_like(q_heads)
    key_mask = column(jnp.where(alive > 0, 0.0, -1000000000.0))
    multiply_first()
    for k in range(MIDDLE):
        turn(k)
    for k in range(SHARED):
        for s in order(PAIRED):
            f_copy(k, partner(s)).start()
    gates(1)
    for k in range(FIRST):
        a_near(k).wait_send()
        a_far(k).wait_send()
    for k in range(MIDDLE):
        b_all(k).wait_send()
    partial_products()
    shared_products()
    for k in range(MIDDLE):
        c_all(k).wait_send()
    for k in range(SHARED):
        f_all(k).wait_send()
    for k in range(LAST):
        attention_inputs(k, close(k))
    for k in range(LAST):
        d_all(k).wait_send()
        g_all(k).wait_send()

    for k in range(LAST):
        e_all(k).wait_recv()
    part = rows // LAST
    for h in range(heads):
        pieces = []
        for q in range(n):
            for k in range(LAST):
                pieces.append(recv_e[k, q].astype(F32)[h * part : (h + 1) * part])
        across = jnp.transpose(jnp.concatenate(pieces, axis=0))
        b_full[:, h * cols : (h + 1) * cols] = (across + key_mask) * LOG2E

    def attend(i, carry):
        parts = []
        for h in range(heads):
            at = slice(h * cols, (h + 1) * cols)
            total = scores[i, :, at] + b_full[:, at]
            e = jnp.exp2(total - jnp.max(total, axis=0, keepdims=True))
            inverse = 1.0 / jnp.sum(e, axis=0, keepdims=True)
            parts.append(mm(vmat[i, h * dim : (h + 1) * dim, :], e.astype(BF16)) * inverse)
        attended = jnp.concatenate(parts, axis=0)
        gated = (gmat[i] * attended).astype(BF16)
        result = mm(out_t[2], gated)
        at = pl.ds(pl.multiple_of(i * cols, cols), cols)
        out_ref[i] = jnp.transpose(zt[:, at].astype(F32) + result).astype(BF16)
        return carry

    lax.fori_loop(0, rows, attend, 0, unroll=8)

    for k in range(LAST):
        e_all(k).wait_send()


def fused(n, pair_rep, residue_mask, crop_length, norm_gain, mult_proj, mixed_gain, mult_out,
          att_gain, att_proj, att_bias, att_out):
    rows, cols, chans = pair_rep.shape
    heads = att_bias.shape[1]
    peers = n // 2
    mine = chans // n
    wide = chans // peers
    vm = pl.BlockSpec(memory_space=pltpu.VMEM)
    hbm = pl.BlockSpec(memory_space=pltpu.HBM)
    phases = 2 * FIRST + 2 * MIDDLE + SHARED + 3 * LAST
    few = mine // 2
    first = pltpu.VMEM((FIRST, 2 * peers, rows // FIRST * wide, cols), BF16)
    first_in = pltpu.VMEM((FIRST, 2 * n, rows // FIRST * wide, cols), BF16)
    back = pltpu.VMEM((MIDDLE, peers, rows // MIDDLE * wide, cols), BF16)
    second = pltpu.VMEM((MIDDLE, peers, 2, rows // MIDDLE * mine, cols), BF16)
    rest = pltpu.VMEM((SHARED, n, 2, rows // SHARED * few, cols), BF16)
    home = pltpu.VMEM((LAST, n, rows // LAST * mine, cols), BF16)
    home_few = pltpu.VMEM((LAST, n, rows // LAST * few, cols), BF16)
    bias = pltpu.VMEM((LAST, heads * rows // LAST, cols), BF16)
    bias_in = pltpu.VMEM((LAST, n, heads * rows // LAST, cols), BF16)

    def far(operand):
        return pltpu.with_memory_space_constraint(operand, pltpu.HBM)

    return pl.pallas_call(
        functools.partial(fused_kernel, n),
        out_shape=jax.ShapeDtypeStruct(pair_rep.shape, BF16),
        in_specs=[hbm, hbm, pl.BlockSpec(memory_space=pltpu.SMEM)] + [hbm] * 8,
        out_specs=vm,
        scratch_shapes=[
            pltpu.VMEM(pair_rep.shape, BF16),
            pltpu.VMEM((1, cols), jnp.int32),
            pltpu.VMEM(norm_gain.shape, F32),
            pltpu.VMEM(mult_proj.shape, BF16),
            pltpu.VMEM(mixed_gain.shape, F32),
            pltpu.VMEM(mult_out.shape, BF16),
            pltpu.VMEM((1, chans), F32),
            pltpu.VMEM(att_proj.shape, BF16),
            pltpu.VMEM((heads, chans), BF16),
            pltpu.VMEM(att_out.shape, BF16),
            pltpu.SemaphoreType.DMA((11,)),
            pltpu.VMEM((chans, rows * cols), BF16),
            pltpu.VMEM((chans, rows * cols), F32),
            pltpu.VMEM((n * rows * mine, cols), F32),
            pltpu.VMEM((n * rows * wide, cols), F32),
            pltpu.VMEM((n * rows * mine, cols), F32),
            pltpu.VMEM((2 * GROUP, chans), F32),
            pltpu.VMEM((cols, heads * cols), F32),
            pltpu.VMEM((rows, cols, chans), BF16),
            pltpu.VMEM((rows, chans, heads * cols), BF16),
            pltpu.VMEM((rows, chans, cols), BF16),
            pltpu.VMEM((rows, chans, cols), F32),
            pltpu.VMEM((rows, cols, heads * cols), F32),
            pltpu.VMEM((2, mult_proj.shape[2], chans), BF16),
            pltpu.VMEM((3, chans, chans), BF16),
            pltpu.VMEM((5, chans, cols), F32),
            pltpu.VMEM((3 * chans, chans), BF16),
            first,
            first_in,
            back,
            back,
            second,
            second,
            rest,
            rest,
            home,
            home,
            home_few,
            home_few,
            bias,
            bias_in,
            pltpu.SemaphoreType.DMA((phases,)),
            pltpu.SemaphoreType.DMA((phases,)),
        ],
        compiler_params=pltpu.CompilerParams(
            collective_id=0, has_side_effects=True, vmem_limit_bytes=48 * 1024 * 1024
        ),
        name="fused_pair",
    )(
        far(pair_rep),
        far(residue_mask.reshape(1, -1)),
        crop_length,
        far(norm_gain),
        far(mult_proj),
        far(mixed_gain),
        far(mult_out),
        far(att_gain.reshape(1, -1)),
        far(att_proj),
        far(att_bias.T),
        far(att_out),
    )


def choose(mesh):
    n = mesh.shape["row"]

    def body(pair_rep, *rest):
        rows, cols, chans = pair_rep.shape
        fits = (
            mesh.shape["col"] == 1
            and n & (n - 1) == 0
            and n > 1
            and chans == n * GROUP
            and rows == GROUP
            and cols == n * rows
            and cols == chans
        )
        if fits:
            return fused(n, pair_rep, *rest)
        return local(pair_rep, *rest)

    return body


def solution(mesh):
    placed = (
        P(("groups", "row"), "col", None),
        P("groups"),
        P("groups"),
        P(),
        P(),
        P(),
        P(),
        P(),
        P(),
        P(),
        P(),
    )
    return jax.shard_map(
        choose(mesh),
        mesh=mesh,
        in_specs=placed,
        out_specs=P(("groups", "row"), "col", None),
        check_vma=False,
    )
```
